256 devices in a mesh: dp: 16 (over y, x), mp: 16 (over z, core).
Axes of the slice: x: 4, y: 4, z: 8, core: 2. Of those that a mesh axis runs over, the one named last changes fastest.
Arguments:
- data_rows: bfloat16 [131072, 2048], P(('dp', 'mp')), may hold values from -32 to 32
- centroids: bfloat16 [12288, 2048], P('mp'), may hold values from -0.75 to 0.75
- block_mask: int32 [16, 1024], P(None, ('dp', 'mp')), may hold values from 0 to 1, as said below
- lower_bound: float32 [16, 131072], P(None, ('dp', 'mp')), may hold values from 0 to 4
Outputs:
- new_centroids: float32 [12288, 2048], P(('mp', 'dp'))
- centroid_shift: float32 [12288], P(('mp', 'dp'))
- log_norm: float32 [131072], P(('dp', 'mp'))
- new_lower: float32 [16, 131072], P(None, ('dp', 'mp'))
The draws below stay inside these ranges and needn't reach their ends.
Inputs may be any that keep to these rules, and one draw needn't show every extreme that they name: `block_mask`: within the 4 blocks of one device (aligned runs along the last dimension), at most 1 are 1 for each shard; for some shard every device has exactly 1.
All inputs are finite; a program needn't handle non-finite values.
Results may differ from the reference program's by a relative error of at most 0.0011.
Values may be sent and summed in bfloat16 or wider, within the bound.
A program may use at most 128 MiB of HBM per device.

```python
import math
import jax
import jax.numpy as jnp
from jax import lax

F = 2048
K = 12288
BLOCK = 128
SLOTS = 1
ROW_DEV = 512
ROWS = 131072
NBLOCKS = 1024
N_MP = 16


def draw_masks(key):
    device_count = ROWS // ROW_DEV
    block_count = ROW_DEV // BLOCK
    base = jax.random.fold_in(key, 11)
    key_bits, key_heavy, key_forced, key_count = jax.random.split(base, 4)
    bits = jax.random.randint(key_bits, (device_count, N_MP, block_count), 0, 1 << 20)
    distinct = bits * block_count + jnp.arange(block_count, dtype=jnp.int32)[None, None, :]
    order = jnp.argsort(distinct, axis=-1)
    block_rank = jnp.argsort(order, axis=-1)
    heavy = jax.random.randint(key_heavy, (N_MP,), 0, 4) == 0
    forced = jax.random.randint(key_forced, (), 0, N_MP)
    heavy = heavy | (jnp.arange(N_MP) == forced)
    chosen_count = jax.random.randint(key_count, (device_count, N_MP), 0, SLOTS + 1)
    chosen_count = jnp.where(heavy[None, :], SLOTS, chosen_count)
    active = (block_rank < chosen_count[:, :, None]).astype(jnp.int32)
    return active.transpose(1, 0, 2).reshape(N_MP, NBLOCKS)


def draw_cents(key):
    base = jax.random.fold_in(key, 23)
    values = 0.125 * jax.random.normal(base, (K, F), jnp.float32)
    return jnp.clip(values, -0.75, 0.75)


def draw_block_mask(key, part):
    return draw_masks(key)


def draw_centroids(key, part):
    return draw_cents(key).astype(jnp.bfloat16)


def draw_data_rows(key, part):
    base = jax.random.fold_in(key, 37)
    key_main = jax.random.fold_in(base, 0)
    values = jnp.clip(jax.random.normal(key_main, (ROWS, F), jnp.float32), -6.0, 6.0)
    return values.astype(jnp.bfloat16)


def steps_of(rng, extent, shards, low, largest):
    def one(axis_at, blocks):
        draws = jax.random.uniform(jax.random.fold_in(jax.random.fold_in(rng, 6), axis_at), (blocks,), jnp.float32, low / len(shards), largest / len(shards))
        return jnp.repeat(jnp.exp(draws), extent[axis_at] // blocks).reshape((-1,) + (1,) * (len(extent) - axis_at - 1))

    level = one(*shards[0])
    for cut in shards[1:]:
        level = level * one(*cut)
    return level


def setup_inputs(seed: int = 0) -> dict:
    key_of = jax.random.split(jax.random.key(seed), 5)
    return {
        "data_rows": draw_data_rows(jax.random.fold_in(key_of[4], 71), 0),
        "centroids": draw_centroids(jax.random.fold_in(key_of[4], 71), 0),
        "block_mask": draw_block_mask(jax.random.fold_in(key_of[4], 71), 0),
        "lower_bound": jnp.clip(4.0 * jax.random.uniform(key_of[3], (N_MP, ROWS), jnp.float32) ** steps_of(key_of[3], (N_MP, ROWS), ((1, 256),), -0.2, 0.2), 0.0, 4.0),
    }


def pack_codes(mask_dev):
    block_count = mask_dev.shape[1]
    block_rank = (jnp.cumsum(mask_dev, axis=1) - 1).astype(jnp.int32)
    slot_ids = jnp.arange(SLOTS, dtype=jnp.int32)
    chosen = (mask_dev[:, None, :] == 1) & (block_rank[:, None, :] == slot_ids[None, :, None])
    labels = jnp.arange(1, block_count + 1, dtype=jnp.int32)
    return lax.optimization_barrier(jnp.sum(jnp.where(chosen, labels[None, None, :], 0), axis=2)).astype(jnp.int32)

def combine_rows(slot_codes, row_top, row_mass, block_count):
    labels = jnp.arange(1, block_count + 1, dtype=jnp.int32)
    is_slot = slot_codes[:, :, None] == labels[None, None, :]
    block_top = lax.optimization_barrier(jnp.max(jnp.where(is_slot[..., None], row_top[:, :, None, :], -1e+30), axis=(0, 1)))
    ceiling = jnp.maximum(block_top, 0.0)
    spread = row_mass[:, :, None, :] * jnp.exp(row_top[:, :, None, :] - ceiling[None, None])
    block_mass = lax.optimization_barrier(jnp.sum(jnp.where(is_slot[..., None], spread, 0.0), axis=(0, 1)))
    row_norm = ceiling + jnp.log(jnp.exp(-ceiling) + block_mass)
    slot_norm = lax.optimization_barrier(jnp.sum(jnp.where(is_slot[..., None], row_norm[None, None], 0.0), axis=2))
    return (row_norm, slot_norm)

def reference(data_rows, centroids, block_mask, lower_bound):
    device_count = ROWS // ROW_DEV
    block_count = ROW_DEV // BLOCK
    shard_width = K // N_MP
    sharpness = 4.0 / math.sqrt(F)
    row_blocks = data_rows.reshape(device_count, block_count, BLOCK, F)
    dev_mask = block_mask.reshape(N_MP, device_count, block_count).transpose(1, 0, 2)
    slot_codes = jax.vmap(pack_codes)(dev_mask)
    cents = centroids.reshape(N_MP, shard_width, F)
    cent_norm = lax.optimization_barrier(jnp.sum(jnp.square(cents.astype(jnp.float32)), axis=2))

    def slot_rows_of(shard):
        code_s = lax.dynamic_index_in_dim(slot_codes, shard, 1, keepdims=False)
        taken = jax.vmap(lambda blk, cde: jnp.take(blk, jnp.maximum(cde - 1, 0), axis=0))(row_blocks, code_s)
        return (jnp.where((code_s > 0)[:, :, None, None], taken, jnp.zeros_like(taken)), code_s)

    def shard_scores(shard):
        slot_rows, code_s = slot_rows_of(shard)
        cent_s = lax.dynamic_index_in_dim(cents, shard, 0, keepdims=False)
        norm_s = lax.dynamic_index_in_dim(cent_norm, shard, 0, keepdims=False)
        products = jnp.dot(slot_rows.reshape(-1, F), cent_s.T, preferred_element_type=jnp.float32)
        scores = sharpness * (2.0 * products - norm_s[None, :])
        scores = scores.reshape(device_count, SLOTS, BLOCK, shard_width)
        is_valid = (code_s > 0)[:, :, None]
        best = lax.optimization_barrier(jnp.max(scores, axis=3))
        row_top = jnp.where(is_valid, best, -1e+30)
        row_mass = jnp.where(is_valid, lax.optimization_barrier(jnp.sum(jnp.exp(scores - best[..., None]), axis=3)), 0.0)
        return (scores, row_top, row_mass)
    all_scores, all_top, all_mass = lax.map(shard_scores, jnp.arange(N_MP, dtype=jnp.int32))
    row_norm, slot_norm = jax.vmap(combine_rows, in_axes=(0, 1, 1, None))(slot_codes, all_top, all_mass, block_count)

    def shard_sums(shard):
        slot_rows, code_s = slot_rows_of(shard)
        scores = lax.dynamic_index_in_dim(all_scores, shard, 0, keepdims=False)
        norm_s = lax.dynamic_index_in_dim(slot_norm, shard, 1, keepdims=False)
        is_valid = (code_s > 0)[:, :, None, None]
        weight = jnp.where(is_valid, jnp.exp(scores - norm_s[..., None]), 0.0)
        counts = lax.optimization_barrier(jnp.sum(weight, axis=(0, 1, 2)))
        weight_half = weight.astype(jnp.bfloat16).reshape(-1, shard_width)
        weighted = jnp.dot(weight_half.T, slot_rows.reshape(-1, F), preferred_element_type=jnp.float32)
        return (weighted, counts)
    weighted, counts = lax.map(shard_sums, jnp.arange(N_MP, dtype=jnp.int32))
    old_cents = cents.astype(jnp.float32)
    updated = (weighted + old_cents) / (counts[..., None] + 1.0)
    movement = jnp.sqrt(lax.optimization_barrier(jnp.sum(jnp.square(updated - old_cents), axis=2)) + 1.0)
    shard_peak = lax.optimization_barrier(jnp.max(movement, axis=1))
    new_lower = lower_bound - shard_peak[:, None]
    return (updated.reshape(K, F), movement.reshape(K), row_norm.reshape(ROWS), new_lower)
```

```python
import functools
import math

import jax
import jax.numpy as jnp
from jax import lax
from jax.experimental import pallas as pl
from jax.experimental.pallas import tpu as pltpu
from jax.sharding import PartitionSpec as P

BLOCK = 128
MESH = pl.DeviceIdType.MESH
NEG = -1e30
F32 = jnp.float32
BF16 = jnp.bfloat16


def rcopy(src, dst, ssem, rsem, dev):
    return pltpu.make_async_remote_copy(
        src_ref=src,
        dst_ref=dst,
        send_sem=ssem,
        recv_sem=rsem,
        device_id=dev,
        device_id_type=MESH,
    )


def kernel(
    data,
    cent,
    codes,
    lower,
    newc,
    shift,
    lognorm,
    newlow,
    full,
    got,
    part,
    selb,
    sel4,
    sc,
    wt,
    sums,
    r1,
    r2,
    r3,
    r4,
    tot,
    cv,
    ct,
    st,
    nrm,
    cnorm,
    cacc,
    cbuf,
    ccol,
    pa,
    pb,
    code_s,
    code_r,
    full_s,
    full_r,
    part_s,
    part_r,
    sel_s,
    sel_r,
    sel4_s,
    sel4_r,
    stat_s,
    stat_r,
    cnt_s,
    cnt_r,
    r1_s,
    r1_r,
    r2_s,
    r2_r,
    r3_s,
    r3_r,
    r4_s,
    r4_r,
    pa_s,
    pa_r,
    pb_s,
    pb_r,
):
    feat = data.shape[1]
    half = feat // 2
    width = cent.shape[0]
    own = width // 16
    sharp = 4.0 / math.sqrt(feat)
    p = lax.axis_index("dp")
    m = lax.axis_index("mp")
    z, c = m // 2, lax.rem(m, 2)
    y, x = p // 4, lax.rem(p, 4)

    def mp_of(dz, j):
        lane = c if j == 0 else 1 - c
        return lax.rem(z + dz + 8, 8) * 2 + lane

    def mp_dev(dz, j):
        return {"mp": mp_of(dz, j)}

    def rows(k, j):
        return pl.ds((k * 2 + j) * BLOCK, BLOCK)

    def slot(h, k, j):
        return got.at[h, rows(k, j), :]

    def mp_at(d):
        return lax.rem(m + d, 16)

    def dp_at(d):
        return lax.rem(p + d, 16)

    barrier = pltpu.get_barrier_semaphore()

    def greet(d, _):
        pl.semaphore_signal(barrier, inc=1, device_id={"mp": mp_at(d)}, device_id_type=MESH)
        pl.semaphore_signal(barrier, inc=1, device_id={"dp": dp_at(d)}, device_id_type=MESH)
        return _

    lax.fori_loop(1, 16, greet, 0)
    cv[m] = codes[...]
    pl.semaphore_wait(barrier, 30)

    order = ((0, 1), (1, 0))
    step = (1, -1)

    def full_copy(way, dist, h):
        src = data.at[:, h * half : (h + 1) * half] if dist == 0 else full.at[way, 0, h]
        return rcopy(
            src,
            full.at[way, dist, h],
            full_s.at[way, dist, h],
            full_r.at[way, dist, h],
            mp_dev(step[way], 0),
        )

    def code_copy(d):
        return rcopy(codes, cv.at[m], code_s.at[d], code_r.at[d], {"mp": mp_at(d)})

    def code_wait(d):
        src = lax.rem(m + 16 - d, 16)
        return rcopy(codes, cv.at[src], code_s.at[d], code_r.at[d], {"mp": src})

    lax.fori_loop(1, 16, lambda d, _: (code_copy(d).start(), _)[1], 0)
    for turn in range(2):
        for way in range(2):
            full_copy(way, 0, order[way][turn]).start()

    def block_of(g, s):
        return jnp.broadcast_to(cv[g, pl.ds(s, 1), :], (BLOCK, BLOCK)).astype(BF16)

    def choose(dst, src, code, first=0):
        for at in range(0, half, BLOCK):
            cols = slice(first + at, first + at + BLOCK)
            out = src[0:BLOCK, cols]
            for b in range(1, src.shape[0] // BLOCK):
                here = code == jnp.asarray(b + 1, BF16)
                out = jnp.where(here, src[b * BLOCK : (b + 1) * BLOCK, cols], out)
            dst[:, at : at + BLOCK] = out

    def part_copy(i, k, h):
        return rcopy(
            part.at[i, h], slot(h, k, 1), part_s.at[i, h], part_r.at[i, h], mp_dev(0, 1)
        )

    at_me, at_partner = block_of(m, m), block_of(m, mp_of(0, 1))
    for h in range(2):
        choose(part.at[0, h], data, at_partner, h * half)
        choose(slot(h, 0, 0), data, at_me, h * half)
    for h in range(2):
        part_copy(0, 0, h).start()

    square = jnp.square(cent[...].astype(F32))
    cnorm[...] = jnp.broadcast_to(jnp.sum(square, axis=1, keepdims=True), cnorm.shape)

    def wait_code(d, _):
        code_wait(d).wait_recv()
        return _

    lax.fori_loop(1, 16, wait_code, 0)

    def turn_codes(g, _):
        for s in range(16):
            ct[s, pl.ds(g, 1), :] = cv[g, s : s + 1, :]
        return _

    lax.fori_loop(0, 16, turn_codes, 0)

    def scores(k):
        where = pl.ds(pl.multiple_of(k * 256, 256), 256)
        nt = (((1,), (1,)), ((), ()))
        prod = lax.dot_general(
            cent[:, :half], got[0, where, :], nt, preferred_element_type=F32
        ) + lax.dot_general(cent[:, half:], got[1, where, :], nt, preferred_element_type=F32)
        score = sharp * (2.0 * prod - cnorm[:, 0:1])
        sc[k] = score
        best = jnp.max(score, axis=0, keepdims=True)
        mass = jnp.sum(jnp.exp(score - best), axis=0, keepdims=True)
        for j in range(2):
            g = mp_of(k, j)
            valid = ct[m, pl.ds(g, 1), :] > 0.0
            lanes = slice(j * BLOCK, (j + 1) * BLOCK)
            st[m, pl.ds(g, 1), :] = jnp.where(valid, best[:, lanes], NEG)
            st[m, pl.ds(16 + g, 1), :] = jnp.where(valid, mass[:, lanes], 0.0)

    def scores_at(ks):
        for k in ks:
            scores(k)

    def keep(way, dist, i, k, h):
        g = mp_of(-step[way] * (dist + 1), 0)
        for j, dst in enumerate((slot(h, k, 0), part.at[i, h])):
            choose(dst, full.at[way, dist, h], block_of(g, mp_of(0, j)))

    def onward(way, dz, j):
        return block_of(mp_of(-step[way] * 2, 0), mp_of(step[way] * dz, j))

    near = {0: 7, 1: 1}
    far = {0: 6, 1: 2}
    third = {0: 5, 1: 3}

    def sel_copy(way, j, h):
        return rcopy(
            selb.at[way, j, h],
            slot(h, third[way], j),
            sel_s.at[way, j, h],
            sel_r.at[way, j, h],
            mp_dev(step[way], j),
        )

    def sel4_copy(way, j):
        return rcopy(
            sel4.at[way, j],
            slot(order[way][0], 4, j),
            sel4_s.at[way, j],
            sel4_r.at[way, j],
            mp_dev(2 * step[way], j),
        )

    for turn in range(2):
        for way in range(2):
            h = order[way][turn]
            full_copy(way, 0, h).wait_recv()
            full_copy(way, 1, h).start()
    for way in range(2):
        for h in range(2):
            keep(way, 0, 1 + way, near[way], h)
        for h in range(2):
            part_copy(1 + way, near[way], h).start()
    for h in range(2):
        part_copy(0, 0, h).wait_recv()
    scores(0)
    for way in range(2):
        for h in range(2):
            part_copy(1 + way, near[way], h).wait_recv()
        scores(near[way])

    for turn in range(2):
        for way in range(2):
            h = order[way][turn]
            full_copy(way, 1, h).wait_recv()
            if turn == 0:
                for j in range(2):
                    choose(sel4.at[way, j], full.at[way, 1, h], onward(way, 2, j))
            for j in range(2):
                choose(selb.at[way, j, h], full.at[way, 1, h], onward(way, 1, j))
            keep(way, 1, 3 + way, far[way], h)
            if turn == 0:
                for j in range(2):
                    sel4_copy(way, j).start()
            for j in range(2):
                sel_copy(way, j, h).start()
            part_copy(3 + way, far[way], h).start()
    for way in range(2):
        for h in range(2):
            part_copy(3 + way, far[way], h).wait_recv()
        scores(far[way])
    for way in range(2):
        for j in range(2):
            sel4_copy(way, j).wait_recv()
    scores(4)
    for way in range(2):
        for j in range(2):
            for h in range(2):
                sel_copy(way, j, h).wait_recv()
        scores(third[way])

    def stat_copy(d):
        return rcopy(st.at[m], st.at[m], stat_s.at[d], stat_r.at[d], {"mp": mp_at(d)})

    def stat_wait(d, _):
        src = lax.rem(m + 16 - d, 16)
        rcopy(st.at[src], st.at[src], stat_s.at[d], stat_r.at[d], {"mp": src}).wait_recv()
        return _

    lax.fori_loop(1, 16, lambda d, _: (stat_copy(d).start(), _)[1], 0)
    lax.fori_loop(1, 16, stat_wait, 0)

    mine = ct[m]
    top = jnp.full(mine.shape, NEG, F32)
    for s in range(16):
        top = jnp.maximum(top, jnp.where(ct[s] == mine, st[s, 0:16, :], NEG))
    ceiling = jnp.maximum(top, 0.0)
    total = jnp.zeros(mine.shape, F32)
    for s in range(16):
        spread = st[s, 16:32, :] * jnp.exp(st[s, 0:16, :] - ceiling)
        total = total + jnp.where(ct[s] == mine, spread, 0.0)
    nrm[...] = ceiling + jnp.log(jnp.exp(-ceiling) + total)

    cacc[...] = jnp.zeros(cacc.shape, F32)

    def weigh(k, _):
        for j in range(2):
            g = mp_of(k, j)
            valid = ct[m, pl.ds(g, 1), :] > 0.0
            norm = nrm[pl.ds(g, 1), :]
            score = sc[k, :, j * BLOCK : (j + 1) * BLOCK]
            weight = jnp.where(valid, jnp.exp(score - norm), 0.0)
            cacc[...] += weight
            at = pl.multiple_of(k * 256 + j * BLOCK, BLOCK)
            wt[:, pl.ds(at, BLOCK)] = weight.astype(BF16)
        return _

    lax.fori_loop(0, 8, weigh, 0)

    quarters = half // 256

    def dp_dev(a, b):
        return {"dp": lax.rem(y + a + 4, 4) * 4 + lax.rem(x + b + 4, 4)}

    first = (x, y)
    second = (y, x)

    def first_dev(h, d):
        return dp_dev(0, d) if h == 0 else dp_dev(d, 0)

    def second_dev(h, d):
        return dp_dev(d, 0) if h == 0 else dp_dev(0, d)

    def plus(v, d):
        return lax.rem(v + d + 4, 4)

    def copy1(h, q, way):
        i = h * quarters + q
        src = sums.at[i, plus(first[h], 2), 2 * way : 2 * way + 2]
        return rcopy(src, r1.at[i, way], r1_s.at[i, way], r1_r.at[i, way], first_dev(h, step[way]))

    def copy2(h, q, way):
        i = h * quarters + q
        src = sums.at[i, plus(first[h], step[way])]
        return rcopy(src, r2.at[i, way], r2_s.at[i, way], r2_r.at[i, way], first_dev(h, step[way]))

    def copy3(h, q, way):
        i = h * quarters + q
        piece = pl.ds(way * (own // 2), own // 2)
        src = sums.at[i, first[h], plus(second[h], 2), piece]
        return rcopy(src, r3.at[i, way], r3_s.at[i, way], r3_r.at[i, way], second_dev(h, step[way]))

    def copy4(h, q, way):
        i = h * quarters + q
        src = sums.at[i, first[h], plus(second[h], step[way])]
        return rcopy(src, r4.at[i, way], r4_s.at[i, way], r4_r.at[i, way], second_dev(h, step[way]))

    def stage1(q):
        for h in range(2):
            i = h * quarters + q
            out = jnp.dot(
                wt[...], got[h, :, q * 256 : (q + 1) * 256], preferred_element_type=F32
            )
            for owner in range(16):
                yy, xx = owner // 4, owner % 4
                a, b = (xx, yy) if h == 0 else (yy, xx)
                sums[i, a, b] = out[owner * own : (owner + 1) * own]
            for way in range(2):
                copy1(h, q, way).start()

    def stage2(q):
        for h in range(2):
            i = h * quarters + q
            for way in range(2):
                copy1(h, q, way).wait_recv()
                a = plus(first[h], step[way])
                sums[i, a, 2 * way : 2 * way + 2] += r1[i, way]
                copy2(h, q, way).start()

    def stage3(q):
        for h in range(2):
            i = h * quarters + q
            for way in range(2):
                copy2(h, q, way).wait_recv()
            sums[i, first[h]] += r2[i, 0] + r2[i, 1]
            for way in range(2):
                copy3(h, q, way).start()

    def stage4(q):
        for h in range(2):
            i = h * quarters + q
            for way in range(2):
                copy3(h, q, way).wait_recv()
                b = plus(second[h], step[way])
                piece = pl.ds(way * (own // 2), own // 2)
                sums[i, first[h], b, piece] += r3[i, way]
                copy4(h, q, way).start()

    def finish(q):
        for h in range(2):
            i = h * quarters + q
            for way in range(2):
                copy4(h, q, way).wait_recv()
            cols = slice(h * half + q * 256, h * half + (q + 1) * 256)
            tot[:, cols] = sums[i, first[h], second[h]] + r4[i, 0] + r4[i, 1]

    def cnt_copy(d):
        return rcopy(cbuf.at[p], cbuf.at[p], cnt_s.at[d], cnt_r.at[d], {"dp": dp_at(d)})

    def cnt_wait(d, _):
        src = lax.rem(p + 16 - d, 16)
        rcopy(cbuf.at[src], cbuf.at[src], cnt_s.at[d], cnt_r.at[d], {"dp": src}).wait_recv()
        return _

    stages = (stage1, stage2, stage3, stage4, finish)
    for t in range(quarters + 4):
        for n, stage in enumerate(stages):
            if 0 <= t - n < quarters:
                stage(t - n)
        if t == 0:
            cbuf[p] = jnp.sum(cacc[...].T, axis=0, keepdims=True)
            lax.fori_loop(1, 16, lambda d, _: (cnt_copy(d).start(), _)[1], 0)
        if t == quarters:
            lax.fori_loop(1, 16, cnt_wait, 0)
            count = jnp.sum(cbuf[...], axis=0)
            ccol[...] = jnp.broadcast_to(count, (BLOCK, width)).T
            number = (lax.broadcasted_iota(jnp.int32, (4, BLOCK), 0) + 1).astype(F32)

            def own_top(s, v):
                here = ct[s, pl.ds(m, 1), :] == number
                return jnp.maximum(v, jnp.where(here, st[s, pl.ds(m, 1), :], NEG))

            best = lax.fori_loop(0, 16, own_top, jnp.full((4, BLOCK), NEG, F32))
            roof = jnp.maximum(best, 0.0)

            def own_mass(s, v):
                here = ct[s, pl.ds(m, 1), :] == number
                spread = st[s, pl.ds(16 + m, 1), :] * jnp.exp(st[s, pl.ds(m, 1), :] - roof)
                return v + jnp.where(here, spread, 0.0)

            mass = lax.fori_loop(0, 16, own_mass, jnp.zeros((4, BLOCK), F32))
            lognorm[...] = roof + jnp.log(jnp.exp(-roof) + mass)

    mine_rows = pl.ds(pl.multiple_of(p * own, own), own)
    old = cent[mine_rows, :].astype(F32)
    denom = ccol[mine_rows, 0:1] + 1.0
    updated = (tot[...] + old) / denom
    newc[...] = updated
    move = jnp.sqrt(jnp.sum(jnp.square(updated - old), axis=1, keepdims=True) + 1.0)
    wide = jnp.broadcast_to(move, (own, BLOCK))
    pa[p] = jnp.max(wide, axis=0, keepdims=True)

    def pa_copy(d):
        return rcopy(pa.at[p], pa.at[p], pa_s.at[d], pa_r.at[d], {"dp": dp_at(d)})

    def pa_wait(d, _):
        src = lax.rem(p + 16 - d, 16)
        rcopy(pa.at[src], pa.at[src], pa_s.at[d], pa_r.at[d], {"dp": src}).wait_recv()
        return _

    lax.fori_loop(1, 16, lambda d, _: (pa_copy(d).start(), _)[1], 0)
    tall = jnp.concatenate([wide, jnp.zeros((BLOCK - own, BLOCK), F32)], axis=0)
    shift[...] = tall.T[0:1, :]
    lax.fori_loop(1, 16, pa_wait, 0)
    pb[m] = jnp.max(pa[...], axis=0)

    def pb_copy(d):
        return rcopy(pb.at[m], pb.at[m], pb_s.at[d], pb_r.at[d], {"mp": mp_at(d)})

    def pb_wait(d, _):
        src = lax.rem(m + 16 - d, 16)
        rcopy(pb.at[src], pb.at[src], pb_s.at[d], pb_r.at[d], {"mp": src}).wait_recv()
        return _

    lax.fori_loop(1, 16, lambda d, _: (pb_copy(d).start(), _)[1], 0)

    for way in range(2):
        for dist in range(2):
            for h in range(2):
                full_copy(way, dist, h).wait_send()
        for j in range(2):
            sel4_copy(way, j).wait_send()
            for h in range(2):
                sel_copy(way, j, h).wait_send()
    for i in range(5):
        for h in range(2):
            part_copy(i, 0, h).wait_send()
    for q in range(quarters):
        for h in range(2):
            for way in range(2):
                for copy in (copy1, copy2, copy3, copy4):
                    copy(h, q, way).wait_send()

    def sent(d, _):
        for copy in (code_copy, stat_copy, cnt_copy, pa_copy):
            copy(d).wait_send()
        return _

    lax.fori_loop(1, 16, sent, 0)
    lax.fori_loop(1, 16, pb_wait, 0)
    for s in range(16):
        peak = pb[s]
        newlow[s : s + 1, :] = lower[s : s + 1, :] - jnp.concatenate([peak] * 4, axis=1)
    lax.fori_loop(1, 16, lambda d, _: (pb_copy(d).wait_send(), _)[1], 0)


def on_device(data_rows, centroids, block_mask, lower_bound):
    rows, feat = data_rows.shape
    blocks = rows // BLOCK
    width = centroids.shape[0]
    half = feat // 2
    own = width // 16
    labels = jnp.arange(1, blocks + 1, dtype=jnp.int32)
    codes = jnp.sum(block_mask * labels[None, :], axis=1, dtype=jnp.int32)
    codes = jnp.broadcast_to(codes[:, None], (16, BLOCK)).astype(F32)
    items = feat // 256
    dma = pltpu.SemaphoreType.DMA
    vmem = pltpu.VMEM
    updated, movement, log_norm, new_lower = pl.pallas_call(
        kernel,
        name="kmeans_step",
        out_shape=(
            jax.ShapeDtypeStruct((own, feat), F32),
            jax.ShapeDtypeStruct((1, BLOCK), F32),
            jax.ShapeDtypeStruct((blocks, BLOCK), F32),
            jax.ShapeDtypeStruct(lower_bound.shape, F32),
        ),
        in_specs=[pl.BlockSpec(memory_space=vmem)] * 4,
        out_specs=[pl.BlockSpec(memory_space=vmem)] * 4,
        scratch_shapes=[
            vmem((2, 2, 2, rows, half), BF16),
            vmem((2, 16 * BLOCK, half), BF16),
            vmem((5, 2, BLOCK, half), BF16),
            vmem((2, 2, 2, BLOCK, half), BF16),
            vmem((2, 2, BLOCK, half), BF16),
            vmem((8, width, 2 * BLOCK), F32),
            vmem((width, 16 * BLOCK), BF16),
            vmem((items, 4, 4, own, 256), F32),
            vmem((items, 2, 2, own, 256), F32),
            vmem((items, 2, 4, own, 256), F32),
            vmem((items, 2, own // 2, 256), F32),
            vmem((items, 2, own, 256), F32),
            vmem((own, feat), F32),
            vmem((16, 16, BLOCK), F32),
            vmem((16, 16, BLOCK), F32),
            vmem((16, 32, BLOCK), F32),
            vmem((16, BLOCK), F32),
            vmem((width, BLOCK), F32),
            vmem((width, BLOCK), F32),
            vmem((16, 1, width), F32),
            vmem((width, BLOCK), F32),
            vmem((16, 1, BLOCK), F32),
            vmem((16, 1, BLOCK), F32),
            dma((16,)),
            dma((16,)),
            dma((2, 2, 2)),
            dma((2, 2, 2)),
            dma((5, 2)),
            dma((5, 2)),
            dma((2, 2, 2)),
            dma((2, 2, 2)),
            dma((2, 2)),
            dma((2, 2)),
            dma((16,)),
            dma((16,)),
            dma((16,)),
            dma((16,)),
            *[dma((items, 2)) for _ in range(8)],
            *[dma((16,)) for _ in range(4)],
        ],
        compiler_params=pltpu.CompilerParams(
            collective_id=0, has_side_effects=True, vmem_limit_bytes=66_000_000
        ),
    )(data_rows, centroids, codes, lower_bound)
    return updated, movement[0, :own], log_norm.reshape(-1), new_lower


def solution(mesh):
    in_specs = (
        P(("dp", "mp"), None),
        P("mp", None),
        P(None, ("dp", "mp")),
        P(None, ("dp", "mp")),
    )
    out_specs = (
        P(("mp", "dp"), None),
        P(("mp", "dp")),
        P(("dp", "mp")),
        P(None, ("dp", "mp")),
    )
    return jax.shard_map(
        on_device, mesh=mesh, in_specs=in_specs, out_specs=out_specs, check_vma=False
    )
```

```python
import functools
import math

import jax
import jax.numpy as jnp
from jax import lax
from jax.experimental import pallas as pl
from jax.experimental.pallas import tpu as pltpu
from jax.sharding import PartitionSpec as P

BLOCK = 128
MESH = pl.DeviceIdType.MESH
NEG = -1e30
F32 = jnp.float32
BF16 = jnp.bfloat16


def rcopy(src, dst, ssem, rsem, dev):
    return pltpu.make_async_remote_copy(
        src_ref=src,
        dst_ref=dst,
        send_sem=ssem,
        recv_sem=rsem,
        device_id=dev,
        device_id_type=MESH,
    )


def kernel(
    data_in,
    cent_in,
    mask_in,
    newc,
    shift,
    lognorm,
    peaks,
    data,
    cent,
    mask,
    full,
    got,
    part,
    selb,
    sel4,
    sc,
    wt,
    sums,
    r1,
    r2,
    r3,
    r4,
    tot,
    cm,
    cv,
    ct,
    st,
    tops,
    nrm,
    cnorm,
    cacc,
    cbuf,
    ccol,
    pa,
    load_s,
    code_s,
    code_r,
    full_s,
    full_r,
    part_s,
    part_r,
    sel_s,
    sel_r,
    sel4_s,
    sel4_r,
    stat_s,
    stat_r,
    cnt_s,
    cnt_r,
    r1_s,
    r1_r,
    r2_s,
    r2_r,
    r3_s,
    r3_r,
    r4_s,
    r4_r,
    pa_s,
    pa_r,
    pb_s,
    pb_r,
):
    half = data.shape[2]
    feat = 2 * half
    width = cent.shape[0]
    own = width // 16
    sharp = 4.0 / math.sqrt(feat)
    p = lax.axis_index("dp")
    m = lax.axis_index("mp")
    z, c = m // 2, lax.rem(m, 2)
    y, x = p // 4, lax.rem(p, 4)

    def mp_of(dz, j):
        lane = c if j == 0 else 1 - c
        return lax.rem(z + dz + 8, 8) * 2 + lane

    def mp_dev(dz, j):
        return {"mp": mp_of(dz, j)}

    def rows(k, j):
        return pl.ds((k * 2 + j) * BLOCK, BLOCK)

    def slot(h, k, j):
        return got.at[h, rows(k, j), :]

    def mp_at(d):
        return lax.rem(m + d, 16)

    def dp_at(d):
        return lax.rem(p + d, 16)

    barrier = pltpu.get_barrier_semaphore()

    def greet(d, _):
        pl.semaphore_signal(barrier, inc=1, device_id={"mp": mp_at(d)}, device_id_type=MESH)
        pl.semaphore_signal(barrier, inc=1, device_id={"dp": dp_at(d)}, device_id_type=MESH)
        return _

    loads = [pltpu.make_async_copy(mask_in, mask, load_s.at[0])]
    for h in range(2):
        src = data_in.at[:, h * half : (h + 1) * half]
        loads.append(pltpu.make_async_copy(src, data.at[h], load_s.at[1 + h]))
    loads.append(pltpu.make_async_copy(cent_in, cent, load_s.at[3]))
    for load in loads:
        load.start()
    lax.fori_loop(1, 16, greet, 0)

    loads[0].wait()
    label = (lax.broadcasted_iota(jnp.int32, mask.shape, 0) + 1).astype(F32)
    code = jnp.sum(mask[...].astype(F32) * label, axis=0, keepdims=True)
    cv[m] = code
    shards = lax.broadcasted_iota(jnp.int32, code.shape, 1)
    for j in range(2):
        here = jnp.sum(jnp.where(shards == mp_of(0, j), code, 0.0), axis=1, keepdims=True)
        cm[j : j + 1, :] = jnp.broadcast_to(here, (1, BLOCK))
    for load in loads[1:3]:
        load.wait()
    pl.semaphore_wait(barrier, 30)

    order = ((0, 1), (1, 0))
    step = (1, -1)

    def full_copy(way, dist, h):
        src = data.at[h] if dist == 0 else full.at[way, 0, h]
        return rcopy(
            src,
            full.at[way, dist, h],
            full_s.at[way, dist, h],
            full_r.at[way, dist, h],
            mp_dev(step[way], 0),
        )

    def code_copy(d):
        return rcopy(cv.at[m], cv.at[m], code_s.at[d], code_r.at[d], {"mp": mp_at(d)})

    def code_wait(d):
        src = lax.rem(m + 16 - d, 16)
        return rcopy(cv.at[src], cv.at[src], code_s.at[d], code_r.at[d], {"mp": src})

    lax.fori_loop(1, 16, lambda d, _: (code_copy(d).start(), _)[1], 0)
    for turn in range(2):
        for way in range(2):
            full_copy(way, 0, order[way][turn]).start()

    def choose(dst, src, code):
        code = jnp.broadcast_to(code, (BLOCK, BLOCK)).astype(BF16)
        for at in range(0, half, BLOCK):
            cols = slice(at, at + BLOCK)
            out = src[0:BLOCK, cols]
            for b in range(1, src.shape[0] // BLOCK):
                here = code == jnp.asarray(b + 1, BF16)
                out = jnp.where(here, src[b * BLOCK : (b + 1) * BLOCK, cols], out)
            dst[:, at : at + BLOCK] = out

    def part_copy(i, k, h):
        return rcopy(
            part.at[i, h], slot(h, k, 1), part_s.at[i, h], part_r.at[i, h], mp_dev(0, 1)
        )

    for h in range(2):
        choose(part.at[0, h], data.at[h], cm[1:2, :])
        choose(slot(h, 0, 0), data.at[h], cm[0:1, :])
    for h in range(2):
        part_copy(0, 0, h).start()

    loads[3].wait()
    square = jnp.square(cent[...].astype(F32))
    cnorm[...] = jnp.broadcast_to(jnp.sum(square, axis=1, keepdims=True), cnorm.shape)

    def wait_code(d, _):
        code_wait(d).wait_recv()
        return _

    lax.fori_loop(1, 16, wait_code, 0)

    codes = cv[:, 0, :]
    for s in range(16):
        column = jnp.broadcast_to(codes[:, s : s + 1], (16, BLOCK))
        for zg in range(8):
            ct[s, zg] = column[2 * zg : 2 * zg + 2]

    def lane_of(j):
        return pl.ds(c if j == 0 else 1 - c, 1)

    def code_of(dz, j, shard):
        return ct[shard, lax.rem(z + dz + 8, 8), lane_of(j), :]

    place = (2, 3, 4, 6, 5, 7, 0, 1)

    def place_of(k):
        at = lax.rem(k + 10, 8)
        return at + jnp.where(at == 5, 1, 0) - jnp.where(at == 6, 1, 0)

    def product(k, h):
        return lax.dot_general(
            cent[:, h * half : (h + 1) * half],
            got[h, k * 256 : (k + 1) * 256, :],
            (((1,), (1,)), ((), ())),
            preferred_element_type=F32,
        )

    def weigh_up(k, prod):
        score = sharp * (2.0 * prod - cnorm[:, 0:1])
        best = jnp.max(score, axis=0, keepdims=True)
        power = jnp.exp(score - best)
        sc[k] = power
        mass = jnp.sum(power, axis=0, keepdims=True)
        whole = best + jnp.log(mass)
        for j in range(2):
            valid = code_of(k, j, m) > 0.0
            lanes = slice(j * BLOCK, (j + 1) * BLOCK)
            tops[k, lane_of(j), :] = best[:, lanes]
            st[m, place[k], lane_of(j), :] = jnp.where(valid, whole[:, lanes], NEG)

    def scores(k):
        weigh_up(k, product(k, 0) + product(k, 1))

    def keep(way, dist, i, k, h):
        for j, dst in enumerate((slot(h, k, 0), part.at[i, h])):
            choose(dst, full.at[way, dist, h], code_of(-step[way] * (dist + 1), 0, mp_of(0, j)))

    def onward(way, dz, j):
        return code_of(-step[way] * 2, 0, mp_of(step[way] * dz, j))

    near = {0: 7, 1: 1}
    far = {0: 6, 1: 2}
    third = {0: 5, 1: 3}

    def sel_copy(way, j, h):
        return rcopy(
            selb.at[way, j, h],
            slot(h, third[way], j),
            sel_s.at[way, j, h],
            sel_r.at[way, j, h],
            mp_dev(step[way], j),
        )

    def sel4_copy(way, j):
        return rcopy(
            sel4.at[way, j],
            slot(order[way][0], 4, j),
            sel4_s.at[way, j],
            sel4_r.at[way, j],
            mp_dev(2 * step[way], j),
        )

    for turn in range(2):
        for way in range(2):
            h = order[way][turn]
            full_copy(way, 0, h).wait_recv()
            full_copy(way, 1, h).start()
    for way in range(2):
        for h in range(2):
            keep(way, 0, 1 + way, near[way], h)
        for h in range(2):
            part_copy(1 + way, near[way], h).start()
    for h in range(2):
        part_copy(0, 0, h).wait_recv()
    scores(0)
    for way in range(2):
        for h in range(2):
            part_copy(1 + way, near[way], h).wait_recv()
        scores(near[way])

    for turn in range(2):
        for way in range(2):
            h = order[way][turn]
            full_copy(way, 1, h).wait_recv()
            if turn == 0:
                for j in range(2):
                    choose(sel4.at[way, j], full.at[way, 1, h], onward(way, 2, j))
            for j in range(2):
                choose(selb.at[way, j, h], full.at[way, 1, h], onward(way, 1, j))
            keep(way, 1, 3 + way, far[way], h)
            if turn == 0:
                for j in range(2):
                    sel4_copy(way, j).start()
            part_copy(3 + way, far[way], h).start()
            for j in range(2 - turn):
                sel_copy(way, j, h).start()
    for way in range(2):
        for h in range(2):
            part_copy(3 + way, far[way], h).wait_recv()
        scores(far[way])
    parts = (slice(0, 6), slice(6, 8))

    def stat_copy(n, d):
        ref = st.at[m, parts[n]]
        return rcopy(ref, ref, stat_s.at[n, d], stat_r.at[n, d], {"mp": mp_at(d)})

    def stat_wait(n, d):
        src = lax.rem(m + 16 - d, 16)
        ref = st.at[src, parts[n]]
        rcopy(ref, ref, stat_s.at[n, d], stat_r.at[n, d], {"mp": src}).wait_recv()

    for way in range(2):
        for j in range(2):
            sel4_copy(way, j).wait_recv()
    scores(4)
    lax.fori_loop(1, 16, lambda d, _: (stat_copy(0, d).start(), _)[1], 0)
    for way in range(2):
        sel_copy(way, 1, order[way][1]).start()
    for turn in range(2):
        for way in range(2):
            h = order[way][turn]
            for j in range(2):
                sel_copy(way, j, h).wait_recv()
            prod = product(third[way], h)
            if turn == 0:
                sc[third[way]] = prod
            else:
                weigh_up(third[way], sc[third[way]] + prod)
    lax.fori_loop(1, 16, lambda d, _: (stat_copy(1, d).start(), _)[1], 0)

    def stats_wait(d, _):
        stat_wait(0, d)
        stat_wait(1, d)
        return _

    lax.fori_loop(1, 16, stats_wait, 0)

    def log_sum(pieces):
        top = functools.reduce(jnp.maximum, pieces)
        ceiling = jnp.maximum(top, 0.0)
        total = functools.reduce(jnp.add, [jnp.exp(piece - ceiling) for piece in pieces])
        return ceiling + jnp.log(jnp.exp(-ceiling) + total)

    def combine(zg, _):
        mine = ct[m, zg]
        pieces = [
            jnp.where(ct[s, zg] == mine, st[s, place_of(zg - s // 2)], NEG) for s in range(16)
        ]
        k = lax.rem(zg - z + 8, 8)
        nrm[zg] = jnp.where(mine > 0.0, jnp.exp(tops[k] - log_sum(pieces)), 0.0)
        return _

    lax.fori_loop(0, 8, combine, 0)

    for k in range(8):
        for j in range(2):
            lanes = slice(j * BLOCK, (j + 1) * BLOCK)
            scale = nrm[lax.rem(z + k, 8), lane_of(j), :]
            weight = sc[k, :, lanes] * scale
            if k == 0 and j == 0:
                cacc[...] = weight
            else:
                cacc[...] += weight
            wt[:, k * 256 + j * BLOCK : k * 256 + (j + 1) * BLOCK] = weight.astype(BF16)

    quarters = half // 256
    items = 2 * quarters

    def dp_dev(a, b):
        return {"dp": lax.rem(y + a + 4, 4) * 4 + lax.rem(x + b + 4, 4)}

    first = (x, y)
    second = (y, x)

    def first_dev(h, d):
        return dp_dev(0, d) if h == 0 else dp_dev(d, 0)

    def second_dev(h, d):
        return dp_dev(d, 0) if h == 0 else dp_dev(0, d)

    def plus(v, d):
        return lax.rem(v + d + 4, 4)

    def copy1(i, way):
        h = i % 2
        src = sums.at[i, plus(first[h], 2), 2 * way : 2 * way + 2]
        return rcopy(src, r1.at[i, way], r1_s.at[i, way], r1_r.at[i, way], first_dev(h, step[way]))

    def copy2(i, way):
        h = i % 2
        src = sums.at[i, plus(first[h], step[way])]
        return rcopy(src, r2.at[i, way], r2_s.at[i, way], r2_r.at[i, way], first_dev(h, step[way]))

    def copy3(i, way):
        h = i % 2
        piece = pl.ds(way * (own // 2), own // 2)
        src = sums.at[i, first[h], plus(second[h], 2), piece]
        return rcopy(src, r3.at[i, way], r3_s.at[i, way], r3_r.at[i, way], second_dev(h, step[way]))

    def copy4(i, way):
        h = i % 2
        src = sums.at[i, first[h], plus(second[h], step[way])]
        return rcopy(src, r4.at[i, way], r4_s.at[i, way], r4_r.at[i, way], second_dev(h, step[way]))

    def stage1(i):
        h, q = i % 2, i // 2
        out = jnp.dot(wt[...], got[h, :, q * 256 : (q + 1) * 256], preferred_element_type=F32)
        for owner in range(16):
            yy, xx = owner // 4, owner % 4
            a, b = (xx, yy) if h == 0 else (yy, xx)
            sums[i, a, b] = out[owner * own : (owner + 1) * own]
        for way in range(2):
            copy1(i, way).start()

    def stage2(i):
        for way in range(2):
            copy1(i, way).wait_recv()
            a = plus(first[i % 2], step[way])
            sums[i, a, 2 * way : 2 * way + 2] += r1[i, way]
            copy2(i, way).start()

    def stage3(i):
        for way in range(2):
            copy2(i, way).wait_recv()
        sums[i, first[i % 2]] += r2[i, 0] + r2[i, 1]
        for way in range(2):
            copy3(i, way).start()

    def stage4(i):
        h = i % 2
        for way in range(2):
            copy3(i, way).wait_recv()
            b = plus(second[h], step[way])
            piece = pl.ds(way * (own // 2), own // 2)
            sums[i, first[h], b, piece] += r3[i, way]
            copy4(i, way).start()

    def finish(i):
        h, q = i % 2, i // 2
        for way in range(2):
            copy4(i, way).wait_recv()
        cols = slice(h * half + q * 256, h * half + (q + 1) * 256)
        tot[:, cols] = sums[i, first[h], second[h]] + r4[i, 0] + r4[i, 1]

    def cnt_copy(d):
        return rcopy(cbuf.at[p], cbuf.at[p], cnt_s.at[d], cnt_r.at[d], {"dp": dp_at(d)})

    def cnt_wait(d, _):
        src = lax.rem(p + 16 - d, 16)
        rcopy(cbuf.at[src], cbuf.at[src], cnt_s.at[d], cnt_r.at[d], {"dp": src}).wait_recv()
        return _

    stages = ((stage1, 0), (stage2, 2), (stage3, 6), (stage4, 8), (finish, 10))
    for t in range(items + 10):
        for stage, late in stages:
            if 0 <= t - late < items:
                stage(t - late)
        if t == 1:
            cbuf[p] = jnp.sum(cacc[...].T, axis=0, keepdims=True)
            lax.fori_loop(1, 16, lambda d, _: (cnt_copy(d).start(), _)[1], 0)
        if t == items - 1:
            lax.fori_loop(1, 16, cnt_wait, 0)
            count = jnp.sum(cbuf[...], axis=0)
            ccol[...] = jnp.broadcast_to(count, (BLOCK, width)).T
            number = (lax.broadcasted_iota(jnp.int32, (4, BLOCK), 0) + 1).astype(F32)
            pieces = []
            for s in range(16):
                here = ct[s, z, lane_of(0), :] == number
                piece = st[s, place_of(z - s // 2), lane_of(0), :]
                pieces.append(jnp.where(here, piece, NEG))
            lognorm[...] = log_sum(pieces)

    mine_rows = pl.ds(pl.multiple_of(p * own, own), own)
    old = cent[mine_rows, :].astype(F32)
    denom = ccol[mine_rows, 0:1] + 1.0
    updated = (tot[...] + old) / denom
    newc[...] = updated
    move = jnp.sqrt(jnp.sum(jnp.square(updated - old), axis=1, keepdims=True) + 1.0)
    wide = jnp.broadcast_to(move, (own, BLOCK))
    pa[p] = jnp.max(wide, axis=0, keepdims=True)

    def pa_copy(d):
        return rcopy(pa.at[p], pa.at[p], pa_s.at[d], pa_r.at[d], {"dp": dp_at(d)})

    def pa_wait(d, _):
        src = lax.rem(p + 16 - d, 16)
        rcopy(pa.at[src], pa.at[src], pa_s.at[d], pa_r.at[d], {"dp": src}).wait_recv()
        return _

    lax.fori_loop(1, 16, lambda d, _: (pa_copy(d).start(), _)[1], 0)
    tall = jnp.concatenate([wide, jnp.zeros((BLOCK - own, BLOCK), F32)], axis=0)
    shift[...] = tall.T[0:1, :]
    lax.fori_loop(1, 16, pa_wait, 0)
    peaks[m] = jnp.max(pa[...], axis=0)

    def pb_copy(d):
        return rcopy(peaks.at[m], peaks.at[m], pb_s.at[d], pb_r.at[d], {"mp": mp_at(d)})

    def pb_wait(d, _):
        src = lax.rem(m + 16 - d, 16)
        rcopy(peaks.at[src], peaks.at[src], pb_s.at[d], pb_r.at[d], {"mp": src}).wait_recv()
        return _

    lax.fori_loop(1, 16, lambda d, _: (pb_copy(d).start(), _)[1], 0)

    for way in range(2):
        for dist in range(2):
            for h in range(2):
                full_copy(way, dist, h).wait_send()
        for j in range(2):
            sel4_copy(way, j).wait_send()
            for h in range(2):
                sel_copy(way, j, h).wait_send()
    for i in range(5):
        for h in range(2):
            part_copy(i, 0, h).wait_send()
    for i in range(items):
        for way in range(2):
            for copy in (copy1, copy2, copy3, copy4):
                copy(i, way).wait_send()

    def sent(d, _):
        for copy in (code_copy, cnt_copy, pa_copy):
            copy(d).wait_send()
        for n in range(2):
            stat_copy(n, d).wait_send()
        return _

    lax.fori_loop(1, 16, sent, 0)
    lax.fori_loop(1, 16, pb_wait, 0)
    lax.fori_loop(1, 16, lambda d, _: (pb_copy(d).wait_send(), _)[1], 0)


def outputs(made, width, logs, peaks, lower, newc, shift, lognorm, newlow):
    newc[...] = made[...]
    shift[...] = width[:, : shift.shape[1]]
    lognorm[...] = logs[...]
    for s in range(16):
        newlow[s : s + 1, :] = lower[s : s + 1, :] - jnp.concatenate([peaks[s]] * 4, axis=1)


def on_device(data_rows, centroids, block_mask, lower_bound):
    rows, feat = data_rows.shape
    blocks = rows // BLOCK
    width = centroids.shape[0]
    half = feat // 2
    own = width // 16
    items = feat // 256
    dma = pltpu.SemaphoreType.DMA
    vmem = pltpu.VMEM
    made, movement, log_norm, peaks = pl.pallas_call(
        kernel,
        name="kmeans_step",
        out_shape=(
            jax.ShapeDtypeStruct((own, feat), F32),
            jax.ShapeDtypeStruct((1, BLOCK), F32),
            jax.ShapeDtypeStruct((blocks, BLOCK), F32),
            jax.ShapeDtypeStruct((16, 1, BLOCK), F32),
        ),
        in_specs=[pl.BlockSpec(memory_space=pl.ANY)] * 3,
        out_specs=[pl.BlockSpec(memory_space=vmem)] * 4,
        scratch_shapes=[
            vmem((2, rows, half), BF16),
            vmem((width, feat), BF16),
            vmem((blocks, 16), jnp.int32),
            vmem((2, 2, 2, rows, half), BF16),
            vmem((2, 16 * BLOCK, half), BF16),
            vmem((5, 2, BLOCK, half), BF16),
            vmem((2, 2, 2, BLOCK, half), BF16),
            vmem((2, 2, BLOCK, half), BF16),
            vmem((8, width, 2 * BLOCK), F32),
            vmem((width, 16 * BLOCK), BF16),
            vmem((items, 4, 4, own, 256), F32),
            vmem((items, 2, 2, own, 256), F32),
            vmem((items, 2, 4, own, 256), F32),
            vmem((items, 2, own // 2, 256), F32),
            vmem((items, 2, own, 256), F32),
            vmem((own, feat), F32),
            vmem((2, BLOCK), F32),
            vmem((16, 1, 16), F32),
            vmem((16, 8, 2, BLOCK), F32),
            vmem((16, 8, 2, BLOCK), F32),
            vmem((8, 2, BLOCK), F32),
            vmem((8, 2, BLOCK), F32),
            vmem((width, BLOCK), F32),
            vmem((width, BLOCK), F32),
            vmem((16, 1, width), F32),
            vmem((width, BLOCK), F32),
            vmem((16, 1, BLOCK), F32),
            dma((4,)),
            dma((16,)),
            dma((16,)),
            dma((2, 2, 2)),
            dma((2, 2, 2)),
            dma((5, 2)),
            dma((5, 2)),
            dma((2, 2, 2)),
            dma((2, 2, 2)),
            dma((2, 2)),
            dma((2, 2)),
            dma((2, 16)),
            dma((2, 16)),
            dma((16,)),
            dma((16,)),
            *[dma((items, 2)) for _ in range(8)],
            *[dma((16,)) for _ in range(4)],
        ],
        compiler_params=pltpu.CompilerParams(
            collective_id=0, has_side_effects=True, vmem_limit_bytes=66_000_000
        ),
    )(data_rows, centroids, block_mask.T)
    updated, movement, log_norm, new_lower = pl.pallas_call(
        outputs,
        name="outputs",
        out_shape=(
            jax.ShapeDtypeStruct(made.shape, F32),
            jax.ShapeDtypeStruct((1, own), F32),
            jax.ShapeDtypeStruct(log_norm.shape, F32),
            jax.ShapeDtypeStruct(lower_bound.shape, F32),
        ),
        in_specs=[pl.BlockSpec(memory_space=vmem)] * 5,
        out_specs=[pl.BlockSpec(memory_space=vmem)] * 4,
    )(made, movement, log_norm, peaks, lower_bound)
    return updated, movement.reshape(-1), log_norm.reshape(-1), new_lower


def solution(mesh):
    in_specs = (
        P(("dp", "mp"), None),
        P("mp", None),
        P(None, ("dp", "mp")),
        P(None, ("dp", "mp")),
    )
    out_specs = (
        P(("mp", "dp"), None),
        P(("mp", "dp")),
        P(("dp", "mp")),
        P(None, ("dp", "mp")),
    )
    return jax.shard_map(
        on_device, mesh=mesh, in_specs=in_specs, out_specs=out_specs, check_vma=False
    )
```

```python
import functools
import math

import jax
import jax.numpy as jnp
from jax import lax
from jax.experimental import pallas as pl
from jax.experimental.pallas import tpu as pltpu
from jax.sharding import PartitionSpec as P

BLOCK = 128
MESH = pl.DeviceIdType.MESH
NEG = -1e30
F32 = jnp.float32
BF16 = jnp.bfloat16


def rcopy(src, dst, ssem, rsem, dev):
    return pltpu.make_async_remote_copy(
        src_ref=src,
        dst_ref=dst,
        send_sem=ssem,
        recv_sem=rsem,
        device_id=dev,
        device_id_type=MESH,
    )


def kernel(
    data_in,
    cent_in,
    mask_in,
    newc,
    shift,
    lognorm,
    peaks,
    data,
    cent,
    mask,
    full,
    got,
    part,
    selb,
    sc,
    wt,
    sums,
    r1,
    r2,
    r3,
    r4,
    te,
    re,
    tot,
    cm,
    cv,
    ct,
    st,
    tops,
    nrm,
    cnorm,
    cacc,
    cbuf,
    csend,
    cret,
    ccol,
    pa,
    load_s,
    code_s,
    code_r,
    cs_s,
    cs_r,
    bc_s,
    bc_r,
    full_s,
    full_r,
    part_s,
    part_r,
    sel_s,
    sel_r,
    stat_s,
    stat_r,
    cnt_s,
    cnt_r,
    r1_s,
    r1_r,
    r2_s,
    r2_r,
    r3_s,
    r3_r,
    r4_s,
    r4_r,
    ret_s,
    ret_r,
    cret_s,
    cret_r,
    pa_s,
    pa_r,
    pb_s,
    pb_r,
):
    half = data.shape[2]
    feat = 2 * half
    width = cent.shape[1]
    own = width // 16
    sharp = 4.0 / math.sqrt(feat)
    p = lax.axis_index("dp")
    m = lax.axis_index("mp")
    z, c = m // 2, lax.rem(m, 2)
    y, x = p // 4, lax.rem(p, 4)
    sign = 1 - 2 * c
    step = (1, -1)
    reach = ((0, 1, -1, 2), (0, 1, -1, -2))
    mine_rows = pl.ds(pl.multiple_of(p * own, own), own)

    def chip(k):
        return lax.rem(z + sign * k + 16, 8)

    def lane(j):
        return c if j == 0 else 1 - c

    def lane_of(j):
        return pl.ds(lane(j), 1)

    def at(k, j):
        return chip(k) * 2 + lane(j)

    def dev(k, j):
        return {"mp": at(k, j)}

    def host(n, k, j):
        if n == 0:
            return at(k, j)
        return at(k + 3, 0) if j == 0 else at(k - 3, 1)

    def slot(n, h, pos, j):
        return got.at[n, h, (pos * 2 + j) * BLOCK : (pos * 2 + j + 1) * BLOCK, :]

    def mp_at(d):
        return lax.rem(m + d, 16)

    def dp_at(d):
        return lax.rem(p + d, 16)

    def each(body):
        lax.fori_loop(1, 16, lambda d, _: (body(d), _)[1], 0)

    barrier = pltpu.get_barrier_semaphore()

    def greet(d):
        pl.semaphore_signal(barrier, inc=1, device_id={"mp": mp_at(d)}, device_id_type=MESH)
        pl.semaphore_signal(barrier, inc=1, device_id={"dp": dp_at(d)}, device_id_type=MESH)

    loads = [pltpu.make_async_copy(mask_in, mask, load_s.at[0])]
    for h in range(2):
        src = data_in.at[:, h * half : (h + 1) * half]
        loads.append(pltpu.make_async_copy(src, data.at[h], load_s.at[1 + h]))
    loads.append(pltpu.make_async_copy(cent_in, cent.at[0], load_s.at[3]))
    for load in loads:
        load.start()
    each(greet)

    loads[0].wait()
    label = (lax.broadcasted_iota(jnp.int32, mask.shape, 0) + 1).astype(F32)
    code = jnp.sum(mask[...].astype(F32) * label, axis=0, keepdims=True)
    cv[m] = code
    shards = lax.broadcasted_iota(jnp.int32, code.shape, 1)
    for n in range(2):
        for j in range(2):
            here = jnp.where(shards == host(n, 0, j), code, 0.0)
            here = jnp.sum(here, axis=1, keepdims=True)
            cm[2 * n + j : 2 * n + j + 1, :] = jnp.broadcast_to(here, (1, BLOCK))
    for load in loads[1:]:
        load.wait()
    pl.semaphore_wait(barrier, 30)

    def code_copy(d):
        return rcopy(cv.at[m], cv.at[m], code_s.at[d], code_r.at[d], {"mp": mp_at(d)})

    def code_wait(d):
        src = lax.rem(m + 16 - d, 16)
        rcopy(cv.at[src], cv.at[src], code_s.at[d], code_r.at[d], {"mp": src}).wait_recv()

    slice_copy = rcopy(cent.at[0, mine_rows], cent.at[1, mine_rows], cs_s.at[0], cs_r.at[0], dev(-3, 0))

    def spread_copy(d):
        ref = cent.at[1, mine_rows]
        return rcopy(ref, ref, bc_s.at[d], bc_r.at[d], {"dp": dp_at(d)})

    def spread_wait(d):
        src = lax.rem(p + 16 - d, 16)
        ref = cent.at[1, pl.ds(pl.multiple_of(src * own, own), own)]
        rcopy(ref, ref, bc_s.at[d], bc_r.at[d], {"dp": src}).wait_recv()

    def full_copy(way, h):
        return rcopy(
            data.at[h], full.at[way, h], full_s.at[way, h], full_r.at[way, h], dev(step[way], 0)
        )

    each(lambda d: code_copy(d).start())
    slice_copy.start()
    for h in range(2):
        for way in range(2):
            full_copy(way, h).start()

    def choose(dst, src, code):
        code = jnp.broadcast_to(code, (BLOCK, BLOCK)).astype(BF16)
        for lanes in range(0, half, BLOCK):
            cols = slice(lanes, lanes + BLOCK)
            out = src[0:BLOCK, cols]
            for b in range(1, src.shape[0] // BLOCK):
                here = code == jnp.asarray(b + 1, BF16)
                out = jnp.where(here, src[b * BLOCK : (b + 1) * BLOCK, cols], out)
            dst[:, cols] = out

    def part_copy(i, n, h):
        return rcopy(
            part.at[i, n, h], slot(n, h, i, 1), part_s.at[i, n, h], part_r.at[i, n, h], dev(0, 1)
        )

    for n in range(2):
        for h in range(2):
            choose(part.at[0, n, h], data.at[h], cm[2 * n + 1 : 2 * n + 2, :])
            choose(slot(n, h, 0, 0), data.at[h], cm[2 * n : 2 * n + 1, :])
    for n in range(2):
        for h in range(2):
            part_copy(0, n, h).start()

    def norms_of(n):
        square = jnp.square(cent[n].astype(F32))
        square = jnp.sum(square, axis=1, keepdims=True)
        cnorm[n] = jnp.broadcast_to(square, cnorm.shape[1:])

    norms_of(0)

    each(code_wait)
    codes = cv[:, 0, :]
    for s in range(16):
        column = jnp.broadcast_to(codes[:, s : s + 1], (16, BLOCK))
        for zg in range(8):
            ct[s, zg] = column[2 * zg : 2 * zg + 2]

    slice_copy.wait_recv()
    each(lambda d: spread_copy(d).start())

    def code_of(k, j, shard):
        return ct[shard, chip(k), lane_of(j), :]

    def product(n, pos, h):
        return lax.dot_general(
            cent[n, :, h * half : (h + 1) * half],
            got[n, h, pos * 256 : (pos + 1) * 256, :],
            (((1,), (1,)), ((), ())),
            preferred_element_type=F32,
        )

    def weigh_up(n, pos, prod):
        score = sharp * (2.0 * prod - cnorm[n, :, 0:1])
        best = jnp.max(score, axis=0, keepdims=True)
        power = jnp.exp(score - best)
        sc[n * 4 + pos] = power.reshape(sc.shape[1:])
        whole = best + jnp.log(jnp.sum(power, axis=0, keepdims=True))
        row = pos * 2 + n
        for j in range(2):
            valid = code_of(reach[n][pos], j, host(n, 0, 0)) > 0.0
            lanes = slice(j * BLOCK, (j + 1) * BLOCK)
            tops[row, lane_of(j), :] = best[:, lanes]
            st[m, row, lane_of(j), :] = jnp.where(valid, whole[:, lanes], NEG)

    def scores(n, pos):
        weigh_up(n, pos, product(n, pos, 0) + product(n, pos, 1))

    def keep(way, h):
        k = -step[way]
        for n in range(2):
            choose(part.at[1 + way, n, h], full.at[way, h], code_of(k, 0, host(n, 0, 1)))
            choose(slot(n, h, 2 - way, 0), full.at[way, h], code_of(k, 0, host(n, 0, 0)))

    def sel_copy(way, j, h):
        n = 1 if way == j else 0
        return rcopy(
            selb.at[way, j, h],
            slot(n, h, 3, j),
            sel_s.at[way, j, h],
            sel_r.at[way, j, h],
            dev(step[way], j),
        )

    def select(way, j, h):
        n = 1 if way == j else 0
        code = code_of(-step[way], 0, host(n, step[way], j))
        choose(selb.at[way, j, h], full.at[way, h], code)

    for h in range(2):
        for way in range(2):
            full_copy(way, h).wait_recv()
            for j in range(2):
                select(way, j, h)
            keep(way, h)
            for j in range(2 - h):
                sel_copy(way, j, h).start()
            for n in range(2):
                part_copy(1 + way, n, h).start()
        if h == 0:
            for hh in range(2):
                part_copy(0, 0, hh).wait_recv()
            scores(0, 0)
    for pos in (1, 2):
        for h in range(2):
            part_copy(pos, 0, h).wait_recv()
        scores(0, pos)
    each(spread_wait)
    norms_of(1)
    for pos in range(3):
        for h in range(2):
            part_copy(pos, 1, h).wait_recv()
        scores(1, pos)

    parts = (slice(0, 6), slice(6, 8))

    def stat_copy(n, d):
        ref = st.at[m, parts[n]]
        return rcopy(ref, ref, stat_s.at[n, d], stat_r.at[n, d], {"mp": mp_at(d)})

    def stat_wait(n, d):
        src = lax.rem(m + 16 - d, 16)
        ref = st.at[src, parts[n]]
        rcopy(ref, ref, stat_s.at[n, d], stat_r.at[n, d], {"mp": src}).wait_recv()

    each(lambda d: stat_copy(0, d).start())
    for way in range(2):
        sel_copy(way, 1, 1).start()
    for h in range(2):
        for way in range(2):
            for j in range(2):
                sel_copy(way, j, h).wait_recv()
        for n in (1, 0):
            prod = product(n, 3, h)
            if h == 0:
                sc[n * 4 + 3] = prod.reshape(sc.shape[1:])
            else:
                weigh_up(n, 3, sc[n * 4 + 3].reshape(width, 256) + prod)
    each(lambda d: stat_copy(1, d).start())
    each(lambda d: stat_wait(0, d))
    each(lambda d: stat_wait(1, d))

    def log_sum(pieces):
        top = functools.reduce(jnp.maximum, pieces)
        ceiling = jnp.maximum(top, 0.0)
        total = functools.reduce(jnp.add, [jnp.exp(piece - ceiling) for piece in pieces])
        return ceiling + jnp.log(jnp.exp(-ceiling) + total)

    near = {0: 0, 1: 1, 7: 2, 2: 3}
    afar = {0: 0, 1: 1, 7: 2, 6: 3}

    def scored(zg, s):
        q, turn = s // 2, 1 - 2 * (s % 2)
        d = (turn * (zg - q)) % 8
        if d in near:
            return s, near[d] * 2
        return ((q - 3 * turn) % 8) * 2 + s % 2, afar[(d + 3) % 8] * 2 + 1

    for zg in range(8):
        for n in range(2):
            mine = ct[host(n, 0, 0), zg]
            pieces = []
            for s in range(16):
                who, row = scored(zg, s)
                pieces.append(jnp.where(ct[s, zg] == mine, st[who, row], NEG))
            nrm[n, zg] = log_sum(pieces)

    def weigh(n):
        for pos in range(4):
            k = reach[n][pos]
            for j in range(2):
                cols = slice(j * BLOCK, (j + 1) * BLOCK)
                gap = tops[pos * 2 + n, lane_of(j), :] - nrm[n, chip(k), lane_of(j), :]
                scale = jnp.where(code_of(k, j, host(n, 0, 0)) > 0.0, jnp.exp(gap), 0.0)
                power = sc[n * 4 + pos, :, :, :, cols].reshape(width, BLOCK)
                weight = power * scale
                if pos == 0 and j == 0:
                    cacc[n] = weight
                else:
                    cacc[n] += weight
                wt[n, :, pos * 256 + j * BLOCK : pos * 256 + (j + 1) * BLOCK] = weight.astype(BF16)

    weigh(1)
    weigh(0)

    each_set = 2 * (half // 256)
    items = 2 * each_set
    held = (sc, sums)
    first = (x, y)
    second = (y, x)

    def dp_dev(a, b):
        return {"dp": lax.rem(y + a + 4, 4) * 4 + lax.rem(x + b + 4, 4)}

    def first_dev(h, d):
        return dp_dev(0, d) if h == 0 else dp_dev(d, 0)

    def second_dev(h, d):
        return dp_dev(d, 0) if h == 0 else dp_dev(0, d)

    def plus(v, d):
        return lax.rem(v + d + 4, 4)

    def item(n):
        i = n % each_set
        return (1 if n < each_set else 0), i, i % 2, i // 2

    def half_rows(way):
        return pl.ds(way * (own // 2), own // 2)

    def copy1(n, way):
        e, i, h, q = item(n)
        src = held[e].at[i, plus(first[h], 2), 2 * way : 2 * way + 2]
        return rcopy(src, r1.at[n, way], r1_s.at[n, way], r1_r.at[n, way], first_dev(h, step[way]))

    def copy2(n, way):
        e, i, h, q = item(n)
        src = held[e].at[i, plus(first[h], step[way])]
        return rcopy(src, r2.at[n, way], r2_s.at[n, way], r2_r.at[n, way], first_dev(h, step[way]))

    def copy3(n, way):
        e, i, h, q = item(n)
        src = held[e].at[i, first[h], plus(second[h], 2), half_rows(way)]
        return rcopy(src, r3.at[n, way], r3_s.at[n, way], r3_r.at[n, way], second_dev(h, step[way]))

    def copy4(n, way):
        e, i, h, q = item(n)
        src = held[e].at[i, first[h], plus(second[h], step[way])]
        return rcopy(src, r4.at[n, way], r4_s.at[n, way], r4_r.at[n, way], second_dev(h, step[way]))

    def back_copy(i):
        return rcopy(te.at[i], re.at[i], ret_s.at[i], ret_r.at[i], dev(3, 0))

    def stage1(n):
        e, i, h, q = item(n)
        out = jnp.dot(wt[e], got[e, h, :, q * 256 : (q + 1) * 256], preferred_element_type=F32)
        for owner in range(16):
            yy, xx = owner // 4, owner % 4
            a, b = (xx, yy) if h == 0 else (yy, xx)
            held[e][i, a, b] = out[owner * own : (owner + 1) * own]
        for way in range(2):
            copy1(n, way).start()

    def stage2(n):
        e, i, h, q = item(n)
        for way in range(2):
            copy1(n, way).wait_recv()
            a = plus(first[h], step[way])
            held[e][i, a, 2 * way : 2 * way + 2] += r1[n, way]
            copy2(n, way).start()

    def stage3(n):
        e, i, h, q = item(n)
        for way in range(2):
            copy2(n, way).wait_recv()
        held[e][i, first[h]] += r2[n, 0] + r2[n, 1]
        for way in range(2):
            copy3(n, way).start()

    def stage4(n):
        e, i, h, q = item(n)
        for way in range(2):
            copy3(n, way).wait_recv()
            held[e][i, first[h], plus(second[h], step[way]), half_rows(way)] += r3[n, way]
            copy4(n, way).start()

    def finish(n):
        e, i, h, q = item(n)
        for way in range(2):
            copy4(n, way).wait_recv()
        value = held[e][i, first[h], second[h]] + r4[n, 0] + r4[n, 1]
        if e == 1:
            te[i] = value
            back_copy(i).start()
        else:
            back_copy(i).wait_recv()
            cols = slice(h * half + q * 256, h * half + (q + 1) * 256)
            tot[:, cols] = value + re[i]

    def cnt_copy(d):
        return rcopy(cbuf.at[p], cbuf.at[p], cnt_s.at[d], cnt_r.at[d], {"dp": dp_at(d)})

    def cnt_wait(d):
        src = lax.rem(p + 16 - d, 16)
        rcopy(cbuf.at[src], cbuf.at[src], cnt_s.at[d], cnt_r.at[d], {"dp": src}).wait_recv()

    count_back = rcopy(csend, cret, cret_s.at[0], cret_r.at[0], dev(3, 0))

    stages = ((stage1, 0), (stage2, 3), (stage3, 8), (stage4, 13), (finish, 18))
    for t in range(items + 18):
        for stage, late in stages:
            if 0 <= t - late < items:
                stage(t - late)
        if t == 3:
            for n in range(2):
                cbuf[p, n] = jnp.sum(cacc[n].T, axis=0, keepdims=True)
            each(lambda d: cnt_copy(d).start())
        if t == items - 1:
            each(cnt_wait)
            csend[...] = jnp.sum(cbuf[:, 1], axis=0)
            count_back.start()
            number = (lax.broadcasted_iota(jnp.int32, (4, BLOCK), 0) + 1).astype(F32)
            pieces = []
            for s in range(16):
                q, turn = s // 2, 1 - 2 * (s % 2)
                d = lax.rem(turn * (z - q) + 16, 8)
                at_home = (d <= 2) | (d == 7)
                who = jnp.where(at_home, s, lax.rem(q - 3 * turn + 8, 8) * 2 + s % 2)
                d = jnp.where(at_home, d, lax.rem(d + 3, 8))
                pos = jnp.where(d == 0, 0, jnp.where(d == 1, 1, jnp.where(d == 7, 2, 3)))
                row = pos * 2 + jnp.where(at_home, 0, 1)
                here = ct[s, z, lane_of(0), :] == number
                pieces.append(jnp.where(here, st[who, row, lane_of(0), :], NEG))
            lognorm[...] = log_sum(pieces)
        if t == items + 4:
            count_back.wait_recv()
            count = jnp.sum(cbuf[:, 0], axis=0) + cret[...]
            ccol[...] = jnp.broadcast_to(count, (BLOCK, width)).T

    old = cent[0, mine_rows, :].astype(F32)
    denom = ccol[mine_rows, 0:1] + 1.0
    updated = (tot[...] + old) / denom
    newc[...] = updated
    move = jnp.sqrt(jnp.sum(jnp.square(updated - old), axis=1, keepdims=True) + 1.0)
    wide = jnp.broadcast_to(move, (own, BLOCK))
    pa[p] = jnp.max(wide, axis=0, keepdims=True)

    def pa_copy(d):
        return rcopy(pa.at[p], pa.at[p], pa_s.at[d], pa_r.at[d], {"dp": dp_at(d)})

    def pa_wait(d):
        src = lax.rem(p + 16 - d, 16)
        rcopy(pa.at[src], pa.at[src], pa_s.at[d], pa_r.at[d], {"dp": src}).wait_recv()

    each(lambda d: pa_copy(d).start())
    tall = jnp.concatenate([wide, jnp.zeros((BLOCK - own, BLOCK), F32)], axis=0)
    shift[...] = tall.T[0:1, :]

    slice_copy.wait_send()
    count_back.wait_send()
    for h in range(2):
        for way in range(2):
            full_copy(way, h).wait_send()
            for j in range(2):
                sel_copy(way, j, h).wait_send()
        for n in range(2):
            for i in range(3):
                part_copy(i, n, h).wait_send()
    for n in range(items):
        for way in range(2):
            for copy in (copy1, copy2, copy3, copy4):
                copy(n, way).wait_send()
    for i in range(each_set):
        back_copy(i).wait_send()

    def sent(d):
        for copy in (code_copy, spread_copy, cnt_copy):
            copy(d).wait_send()
        for n in range(2):
            stat_copy(n, d).wait_send()

    each(sent)

    each(pa_wait)
    peaks[m] = jnp.max(pa[...], axis=0)

    def pb_copy(d):
        return rcopy(peaks.at[m], peaks.at[m], pb_s.at[d], pb_r.at[d], {"mp": mp_at(d)})

    def pb_wait(d):
        src = lax.rem(m + 16 - d, 16)
        rcopy(peaks.at[src], peaks.at[src], pb_s.at[d], pb_r.at[d], {"mp": src}).wait_recv()

    each(lambda d: pb_copy(d).start())
    each(lambda d: pa_copy(d).wait_send())
    each(pb_wait)
    each(lambda d: pb_copy(d).wait_send())


def outputs(made, width, logs, peaks, lower, newc, shift, lognorm, newlow):
    newc[...] = made[...]
    shift[...] = width[:, : shift.shape[1]]
    lognorm[...] = logs[...]
    for s in range(16):
        newlow[s : s + 1, :] = lower[s : s + 1, :] - jnp.concatenate([peaks[s]] * 4, axis=1)


def on_device(data_rows, centroids, block_mask, lower_bound):
    rows, feat = data_rows.shape
    blocks = rows // BLOCK
    width = centroids.shape[0]
    half = feat // 2
    own = width // 16
    items = 2 * (feat // 256)
    dma = pltpu.SemaphoreType.DMA
    vmem = pltpu.VMEM
    made, movement, log_norm, peaks = pl.pallas_call(
        kernel,
        name="kmeans_step",
        out_shape=(
            jax.ShapeDtypeStruct((own, feat), F32),
            jax.ShapeDtypeStruct((1, BLOCK), F32),
            jax.ShapeDtypeStruct((blocks, BLOCK), F32),
            jax.ShapeDtypeStruct((16, 1, BLOCK), F32),
        ),
        in_specs=[pl.BlockSpec(memory_space=pl.ANY)] * 3,
        out_specs=[pl.BlockSpec(memory_space=vmem)] * 4,
        scratch_shapes=[
            vmem((2, rows, half), BF16),
            vmem((2, width, feat), BF16),
            vmem((blocks, 16), jnp.int32),
            vmem((2, 2, rows, half), BF16),
            vmem((2, 2, 8 * BLOCK, half), BF16),
            vmem((3, 2, 2, BLOCK, half), BF16),
            vmem((2, 2, 2, BLOCK, half), BF16),
            vmem((8, 4, 4, own, 256), F32),
            vmem((2, width, 8 * BLOCK), BF16),
            vmem((8, 4, 4, own, 256), F32),
            vmem((items, 2, 2, own, 256), F32),
            vmem((items, 2, 4, own, 256), F32),
            vmem((items, 2, own // 2, 256), F32),
            vmem((items, 2, own, 256), F32),
            vmem((8, own, 256), F32),
            vmem((8, own, 256), F32),
            vmem((own, feat), F32),
            vmem((4, BLOCK), F32),
            vmem((16, 1, 16), F32),
            vmem((16, 8, 2, BLOCK), F32),
            vmem((16, 8, 2, BLOCK), F32),
            vmem((8, 2, BLOCK), F32),
            vmem((2, 8, 2, BLOCK), F32),
            vmem((2, width, BLOCK), F32),
            vmem((2, width, BLOCK), F32),
            vmem((16, 2, 1, width), F32),
            vmem((1, width), F32),
            vmem((1, width), F32),
            vmem((width, BLOCK), F32),
            vmem((16, 1, BLOCK), F32),
            dma((4,)),
            dma((16,)),
            dma((16,)),
            dma((1,)),
            dma((1,)),
            dma((16,)),
            dma((16,)),
            dma((2, 2)),
            dma((2, 2)),
            dma((3, 2, 2)),
            dma((3, 2, 2)),
            dma((2, 2, 2)),
            dma((2, 2, 2)),
            dma((2, 16)),
            dma((2, 16)),
            dma((16,)),
            dma((16,)),
            *[dma((items, 2)) for _ in range(8)],
            dma((8,)),
            dma((8,)),
            dma((1,)),
            dma((1,)),
            *[dma((16,)) for _ in range(4)],
        ],
        compiler_params=pltpu.CompilerParams(
            collective_id=0, has_side_effects=True, vmem_limit_bytes=66_000_000
        ),
    )(data_rows, centroids, block_mask.T)
    updated, movement, log_norm, new_lower = pl.pallas_call(
        outputs,
        name="outputs",
        out_shape=(
            jax.ShapeDtypeStruct(made.shape, F32),
            jax.ShapeDtypeStruct((1, own), F32),
            jax.ShapeDtypeStruct(log_norm.shape, F32),
            jax.ShapeDtypeStruct(lower_bound.shape, F32),
        ),
        in_specs=[pl.BlockSpec(memory_space=vmem)] * 5,
        out_specs=[pl.BlockSpec(memory_space=vmem)] * 4,
    )(made, movement, log_norm, peaks, lower_bound)
    return updated, movement.reshape(-1), log_norm.reshape(-1), new_lower


def solution(mesh):
    in_specs = (
        P(("dp", "mp"), None),
        P("mp", None),
        P(None, ("dp", "mp")),
        P(None, ("dp", "mp")),
    )
    out_specs = (
        P(("mp", "dp"), None),
        P(("mp", "dp")),
        P(("dp", "mp")),
        P(None, ("dp", "mp")),
    )
    return jax.shard_map(
        on_device, mesh=mesh, in_specs=in_specs, out_specs=out_specs, check_vma=False
    )
```

```python
import functools
import math

import jax
import jax.numpy as jnp
from jax import lax
from jax.experimental import pallas as pl
from jax.experimental.pallas import tpu as pltpu
from jax.sharding import PartitionSpec as P

BLOCK = 128
MESH = pl.DeviceIdType.MESH
NEG = -1e30
F32 = jnp.float32
BF16 = jnp.bfloat16


def rcopy(src, dst, ssem, rsem, dev):
    return pltpu.make_async_remote_copy(
        src_ref=src,
        dst_ref=dst,
        send_sem=ssem,
        recv_sem=rsem,
        device_id=dev,
        device_id_type=MESH,
    )


def kernel(
    data_in,
    cent_in,
    mask_in,
    newc,
    shift,
    lognorm,
    peaks,
    data,
    cent,
    mask,
    full,
    got,
    part,
    selb,
    sc,
    wt,
    sums,
    s1,
    r1,
    r2,
    r3,
    r4,
    te,
    re,
    tot,
    cm,
    cv,
    ct,
    st,
    tops,
    nrm,
    cnorm,
    cacc,
    cbuf,
    csend,
    cret,
    ccol,
    pa,
    load_s,
    code_s,
    code_r,
    cs_s,
    cs_r,
    bc_s,
    bc_r,
    full_s,
    full_r,
    part_s,
    part_r,
    sel_s,
    sel_r,
    stat_s,
    stat_r,
    cnt_s,
    cnt_r,
    r1_s,
    r1_r,
    r2_s,
    r2_r,
    r3_s,
    r3_r,
    r4_s,
    r4_r,
    ret_s,
    ret_r,
    cret_s,
    cret_r,
    pa_s,
    pa_r,
    pb_s,
    pb_r,
):
    half = data.shape[2]
    feat = 2 * half
    width = cent.shape[1]
    own = width // 16
    sharp = 4.0 / math.sqrt(feat)
    p = lax.axis_index("dp")
    m = lax.axis_index("mp")
    z, c = m // 2, lax.rem(m, 2)
    y, x = p // 4, lax.rem(p, 4)
    sign = 1 - 2 * c
    step = (1, -1)
    reach = ((0, 1, -1, 2), (0, 1, -1, -2))
    mine_rows = pl.ds(pl.multiple_of(p * own, own), own)

    def chip(k):
        return lax.rem(z + sign * k + 16, 8)

    def lane(j):
        return c if j == 0 else 1 - c

    def lane_of(j):
        return pl.ds(lane(j), 1)

    def at(k, j):
        return chip(k) * 2 + lane(j)

    def dev(k, j):
        return {"mp": at(k, j)}

    def host(n, k, j):
        if n == 0:
            return at(k, j)
        return at(k + 3, 0) if j == 0 else at(k - 3, 1)

    def slot(n, h, pos, j):
        return got.at[n, h, (pos * 2 + j) * BLOCK : (pos * 2 + j + 1) * BLOCK, :]

    def mp_at(d):
        return lax.rem(m + d, 16)

    def dp_at(d):
        return lax.rem(p + d, 16)

    def each(body):
        lax.fori_loop(1, 16, lambda d, _: (body(d), _)[1], 0)

    barrier = pltpu.get_barrier_semaphore()

    def greet(d):
        pl.semaphore_signal(barrier, inc=1, device_id={"mp": mp_at(d)}, device_id_type=MESH)
        pl.semaphore_signal(barrier, inc=1, device_id={"dp": dp_at(d)}, device_id_type=MESH)

    loads = [pltpu.make_async_copy(mask_in, mask, load_s.at[0])]
    for h in range(2):
        src = data_in.at[:, h * half : (h + 1) * half]
        loads.append(pltpu.make_async_copy(src, data.at[h], load_s.at[1 + h]))
    loads.append(pltpu.make_async_copy(cent_in, cent.at[0], load_s.at[3]))
    for load in loads:
        load.start()
    each(greet)

    loads[0].wait()
    label = (lax.broadcasted_iota(jnp.int32, mask.shape, 0) + 1).astype(F32)
    code = jnp.sum(mask[...].astype(F32) * label, axis=0, keepdims=True)
    cv[m] = code
    shards = lax.broadcasted_iota(jnp.int32, code.shape, 1)
    for n in range(2):
        for j in range(2):
            here = jnp.where(shards == host(n, 0, j), code, 0.0)
            here = jnp.sum(here, axis=1, keepdims=True)
            cm[2 * n + j : 2 * n + j + 1, :] = jnp.broadcast_to(here, (1, BLOCK))
    for load in loads[1:]:
        load.wait()
    pl.semaphore_wait(barrier, 30)

    def code_copy(d):
        return rcopy(cv.at[m], cv.at[m], code_s.at[d], code_r.at[d], {"mp": mp_at(d)})

    def code_wait(d):
        src = lax.rem(m + 16 - d, 16)
        rcopy(cv.at[src], cv.at[src], code_s.at[d], code_r.at[d], {"mp": src}).wait_recv()

    slice_copy = rcopy(cent.at[0, mine_rows], cent.at[1, mine_rows], cs_s.at[0], cs_r.at[0], dev(-3, 0))

    def spread_copy(d):
        ref = cent.at[1, mine_rows]
        return rcopy(ref, ref, bc_s.at[d], bc_r.at[d], {"dp": dp_at(d)})

    def spread_wait(d):
        src = lax.rem(p + 16 - d, 16)
        ref = cent.at[1, pl.ds(pl.multiple_of(src * own, own), own)]
        rcopy(ref, ref, bc_s.at[d], bc_r.at[d], {"dp": src}).wait_recv()

    def full_copy(way, h):
        return rcopy(
            data.at[h], full.at[way, h], full_s.at[way, h], full_r.at[way, h], dev(step[way], 0)
        )

    each(lambda d: code_copy(d).start())
    slice_copy.start()
    for h in range(2):
        for way in range(2):
            full_copy(way, h).start()

    def choose(dst, src, code):
        code = jnp.broadcast_to(code, (BLOCK, BLOCK)).astype(BF16)
        for lanes in range(0, half, BLOCK):
            cols = slice(lanes, lanes + BLOCK)
            out = src[0:BLOCK, cols]
            for b in range(1, src.shape[0] // BLOCK):
                here = code == jnp.asarray(b + 1, BF16)
                out = jnp.where(here, src[b * BLOCK : (b + 1) * BLOCK, cols], out)
            dst[:, cols] = out

    def part_copy(i, n, h):
        return rcopy(
            part.at[i, n, h], slot(n, h, i, 1), part_s.at[i, n, h], part_r.at[i, n, h], dev(0, 1)
        )

    for n in range(2):
        for h in range(2):
            choose(part.at[0, n, h], data.at[h], cm[2 * n + 1 : 2 * n + 2, :])
            choose(slot(n, h, 0, 0), data.at[h], cm[2 * n : 2 * n + 1, :])
    for n in range(2):
        for h in range(2):
            part_copy(0, n, h).start()

    def norms_of(n):
        square = jnp.square(cent[n].astype(F32))
        square = jnp.sum(square, axis=1, keepdims=True)
        cnorm[n] = jnp.broadcast_to(square, cnorm.shape[1:])

    norms_of(0)

    each(code_wait)
    codes = cv[:, 0, :]
    for s in range(16):
        column = jnp.broadcast_to(codes[:, s : s + 1], (16, BLOCK))
        for zg in range(8):
            ct[s, zg] = column[2 * zg : 2 * zg + 2]

    slice_copy.wait_recv()
    each(lambda d: spread_copy(d).start())

    def code_of(k, j, shard):
        return ct[shard, chip(k), lane_of(j), :]

    def product(n, pos, h):
        return lax.dot_general(
            cent[n, :, h * half : (h + 1) * half],
            got[n, h, pos * 256 : (pos + 1) * 256, :],
            (((1,), (1,)), ((), ())),
            preferred_element_type=F32,
        )

    def weigh_up(n, pos, prod):
        score = sharp * (2.0 * prod - cnorm[n, :, 0:1])
        best = jnp.max(score, axis=0, keepdims=True)
        power = jnp.exp(score - best)
        sc[n * 4 + pos] = power.reshape(sc.shape[1:])
        whole = best + jnp.log(jnp.sum(power, axis=0, keepdims=True))
        row = pos * 2 + n
        for j in range(2):
            valid = code_of(reach[n][pos], j, host(n, 0, 0)) > 0.0
            lanes = slice(j * BLOCK, (j + 1) * BLOCK)
            tops[row, lane_of(j), :] = best[:, lanes]
            st[m, row, lane_of(j), :] = jnp.where(valid, whole[:, lanes], NEG)

    def scores(n, pos):
        weigh_up(n, pos, product(n, pos, 0) + product(n, pos, 1))

    def keep(way, h):
        k = -step[way]
        for n in range(2):
            choose(part.at[1 + way, n, h], full.at[way, h], code_of(k, 0, host(n, 0, 1)))
            choose(slot(n, h, 2 - way, 0), full.at[way, h], code_of(k, 0, host(n, 0, 0)))

    def sel_copy(way, j, h):
        n = 1 if way == j else 0
        return rcopy(
            selb.at[way, j, h],
            slot(n, h, 3, j),
            sel_s.at[way, j, h],
            sel_r.at[way, j, h],
            dev(step[way], j),
        )

    def select(way, j, h):
        n = 1 if way == j else 0
        code = code_of(-step[way], 0, host(n, step[way], j))
        choose(selb.at[way, j, h], full.at[way, h], code)

    for h in range(2):
        for way in range(2):
            full_copy(way, h).wait_recv()
            for j in range(2):
                select(way, j, h)
            keep(way, h)
            for j in range(2 - h):
                sel_copy(way, j, h).start()
            for n in range(2):
                part_copy(1 + way, n, h).start()
        if h == 0:
            for hh in range(2):
                part_copy(0, 0, hh).wait_recv()
            scores(0, 0)
    for pos in (1, 2):
        for h in range(2):
            part_copy(pos, 0, h).wait_recv()
        scores(0, pos)
    each(spread_wait)
    norms_of(1)
    for pos in range(3):
        for h in range(2):
            part_copy(pos, 1, h).wait_recv()
        scores(1, pos)

    parts = (slice(0, 6), slice(6, 8))

    def stat_copy(n, d):
        ref = st.at[m, parts[n]]
        return rcopy(ref, ref, stat_s.at[n, d], stat_r.at[n, d], {"mp": mp_at(d)})

    def stat_wait(n, d):
        src = lax.rem(m + 16 - d, 16)
        ref = st.at[src, parts[n]]
        rcopy(ref, ref, stat_s.at[n, d], stat_r.at[n, d], {"mp": src}).wait_recv()

    each(lambda d: stat_copy(0, d).start())
    for way in range(2):
        sel_copy(way, 1, 1).start()
    for h in range(2):
        for way in range(2):
            for j in range(2):
                sel_copy(way, j, h).wait_recv()
        for n in (1, 0):
            prod = product(n, 3, h)
            if h == 0:
                sc[n * 4 + 3] = prod.reshape(sc.shape[1:])
            else:
                weigh_up(n, 3, sc[n * 4 + 3].reshape(width, 256) + prod)
    each(lambda d: stat_copy(1, d).start())
    each(lambda d: stat_wait(0, d))
    each(lambda d: stat_wait(1, d))

    def log_sum(pieces):
        top = functools.reduce(jnp.maximum, pieces)
        ceiling = jnp.maximum(top, 0.0)
        total = functools.reduce(jnp.add, [jnp.exp(piece - ceiling) for piece in pieces])
        return ceiling + jnp.log(jnp.exp(-ceiling) + total)

    near = {0: 0, 1: 1, 7: 2, 2: 3}
    afar = {0: 0, 1: 1, 7: 2, 6: 3}

    def scored(zg, s):
        q, turn = s // 2, 1 - 2 * (s % 2)
        d = (turn * (zg - q)) % 8
        if d in near:
            return s, near[d] * 2
        return ((q - 3 * turn) % 8) * 2 + s % 2, afar[(d + 3) % 8] * 2 + 1

    for zg in range(8):
        for n in range(2):
            mine = ct[host(n, 0, 0), zg]
            pieces = []
            for s in range(16):
                who, row = scored(zg, s)
                pieces.append(jnp.where(ct[s, zg] == mine, st[who, row], NEG))
            nrm[n, zg] = log_sum(pieces)

    def weigh(n):
        for pos in range(4):
            k = reach[n][pos]
            for j in range(2):
                cols = slice(j * BLOCK, (j + 1) * BLOCK)
                gap = tops[pos * 2 + n, lane_of(j), :] - nrm[n, chip(k), lane_of(j), :]
                scale = jnp.where(code_of(k, j, host(n, 0, 0)) > 0.0, jnp.exp(gap), 0.0)
                power = sc[n * 4 + pos, :, :, :, cols].reshape(width, BLOCK)
                weight = power * scale
                if pos == 0 and j == 0:
                    cacc[n] = weight
                else:
                    cacc[n] += weight
                wt[n, :, pos * 256 + j * BLOCK : pos * 256 + (j + 1) * BLOCK] = weight.astype(BF16)

    weigh(1)
    weigh(0)

    each_set = 2 * (half // 256)
    items = 2 * each_set
    held = (sc, sums)
    first = (x, y)
    second = (y, x)

    def dp_dev(a, b):
        return {"dp": lax.rem(y + a + 4, 4) * 4 + lax.rem(x + b + 4, 4)}

    def first_dev(h, d):
        return dp_dev(0, d) if h == 0 else dp_dev(d, 0)

    def second_dev(h, d):
        return dp_dev(d, 0) if h == 0 else dp_dev(0, d)

    def plus(v, d):
        return lax.rem(v + d + 4, 4)

    def item(n):
        i = n % each_set
        return (1 if n < each_set else 0), i, i % 2, i // 2

    def half_rows(way):
        return pl.ds(way * (own // 2), own // 2)

    def copy1(n, way):
        h = item(n)[2]
        return rcopy(s1.at[n, way], r1.at[n, way], r1_s.at[n, way], r1_r.at[n, way], first_dev(h, step[way]))

    def copy2(n, way):
        e, i, h, q = item(n)
        src = held[e].at[i, plus(first[h], step[way])]
        return rcopy(src, r2.at[n, way], r2_s.at[n, way], r2_r.at[n, way], first_dev(h, step[way]))

    def copy3(n, way):
        e, i, h, q = item(n)
        src = held[e].at[i, first[h], plus(second[h], 2), half_rows(way)]
        return rcopy(src, r3.at[n, way], r3_s.at[n, way], r3_r.at[n, way], second_dev(h, step[way]))

    def copy4(n, way):
        e, i, h, q = item(n)
        src = held[e].at[i, first[h], plus(second[h], step[way])]
        return rcopy(src, r4.at[n, way], r4_s.at[n, way], r4_r.at[n, way], second_dev(h, step[way]))

    def back_copy(i):
        return rcopy(te.at[i], re.at[i], ret_s.at[i], ret_r.at[i], dev(3, 0))

    def stage1(n):
        e, i, h, q = item(n)
        out = jnp.dot(wt[e], got[e, h, :, q * 256 : (q + 1) * 256], preferred_element_type=F32)
        for owner in range(16):
            yy, xx = owner // 4, owner % 4
            a, b = (xx, yy) if h == 0 else (yy, xx)
            held[e][i, a, b] = out[owner * own : (owner + 1) * own]
        for way in range(2):
            s1[n, way] = held[e][i, plus(first[h], 2), 2 * way : 2 * way + 2].astype(BF16)
        for way in range(2):
            copy1(n, way).start()

    def stage2(n):
        e, i, h, q = item(n)
        for way in range(2):
            copy1(n, way).wait_recv()
            a = plus(first[h], step[way])
            held[e][i, a, 2 * way : 2 * way + 2] += r1[n, way].astype(F32)
            copy2(n, way).start()

    def stage3(n):
        e, i, h, q = item(n)
        for way in range(2):
            copy2(n, way).wait_recv()
        held[e][i, first[h]] += r2[n, 0] + r2[n, 1]
        for way in range(2):
            copy3(n, way).start()

    def stage4(n):
        e, i, h, q = item(n)
        for way in range(2):
            copy3(n, way).wait_recv()
            held[e][i, first[h], plus(second[h], step[way]), half_rows(way)] += r3[n, way]
            copy4(n, way).start()

    def finish(n):
        e, i, h, q = item(n)
        for way in range(2):
            copy4(n, way).wait_recv()
        value = held[e][i, first[h], second[h]] + r4[n, 0] + r4[n, 1]
        if e == 1:
            te[i] = value
            back_copy(i).start()
        else:
            back_copy(i).wait_recv()
            cols = slice(h * half + q * 256, h * half + (q + 1) * 256)
            tot[:, cols] = value + re[i]

    def cnt_copy(d):
        return rcopy(cbuf.at[p], cbuf.at[p], cnt_s.at[d], cnt_r.at[d], {"dp": dp_at(d)})

    def cnt_wait(d):
        src = lax.rem(p + 16 - d, 16)
        rcopy(cbuf.at[src], cbuf.at[src], cnt_s.at[d], cnt_r.at[d], {"dp": src}).wait_recv()

    count_back = rcopy(csend, cret, cret_s.at[0], cret_r.at[0], dev(3, 0))

    stages = ((stage1, 0), (stage2, 3), (stage3, 8), (stage4, 13), (finish, 18))
    for t in range(items + 18):
        for stage, late in stages:
            if 0 <= t - late < items:
                stage(t - late)
        if t == 3:
            for n in range(2):
                cbuf[p, n] = jnp.sum(cacc[n].T, axis=0, keepdims=True)
            each(lambda d: cnt_copy(d).start())
        if t == items - 1:
            each(cnt_wait)
            csend[...] = jnp.sum(cbuf[:, 1], axis=0)
            count_back.start()
            number = (lax.broadcasted_iota(jnp.int32, (4, BLOCK), 0) + 1).astype(F32)
            pieces = []
            for s in range(16):
                q, turn = s // 2, 1 - 2 * (s % 2)
                d = lax.rem(turn * (z - q) + 16, 8)
                at_home = (d <= 2) | (d == 7)
                who = jnp.where(at_home, s, lax.rem(q - 3 * turn + 8, 8) * 2 + s % 2)
                d = jnp.where(at_home, d, lax.rem(d + 3, 8))
                pos = jnp.where(d == 0, 0, jnp.where(d == 1, 1, jnp.where(d == 7, 2, 3)))
                row = pos * 2 + jnp.where(at_home, 0, 1)
                here = ct[s, z, lane_of(0), :] == number
                pieces.append(jnp.where(here, st[who, row, lane_of(0), :], NEG))
            lognorm[...] = log_sum(pieces)
        if t == items + 4:
            count_back.wait_recv()
            count = jnp.sum(cbuf[:, 0], axis=0) + cret[...]
            ccol[...] = jnp.broadcast_to(count, (BLOCK, width)).T

    old = cent[0, mine_rows, :].astype(F32)
    denom = ccol[mine_rows, 0:1] + 1.0
    updated = (tot[...] + old) / denom
    newc[...] = updated
    move = jnp.sqrt(jnp.sum(jnp.square(updated - old), axis=1, keepdims=True) + 1.0)
    wide = jnp.broadcast_to(move, (own, BLOCK))
    pa[p] = jnp.max(wide, axis=0, keepdims=True)

    def pa_copy(d):
        return rcopy(pa.at[p], pa.at[p], pa_s.at[d], pa_r.at[d], {"dp": dp_at(d)})

    def pa_wait(d):
        src = lax.rem(p + 16 - d, 16)
        rcopy(pa.at[src], pa.at[src], pa_s.at[d], pa_r.at[d], {"dp": src}).wait_recv()

    each(lambda d: pa_copy(d).start())
    tall = jnp.concatenate([wide, jnp.zeros((BLOCK - own, BLOCK), F32)], axis=0)
    shift[...] = tall.T[0:1, :]

    slice_copy.wait_send()
    count_back.wait_send()
    for h in range(2):
        for way in range(2):
            full_copy(way, h).wait_send()
            for j in range(2):
                sel_copy(way, j, h).wait_send()
        for n in range(2):
            for i in range(3):
                part_copy(i, n, h).wait_send()
    for n in range(items):
        for way in range(2):
            for copy in (copy1, copy2, copy3, copy4):
                copy(n, way).wait_send()
    for i in range(each_set):
        back_copy(i).wait_send()

    def sent(d):
        for copy in (code_copy, spread_copy, cnt_copy):
            copy(d).wait_send()
        for n in range(2):
            stat_copy(n, d).wait_send()

    each(sent)

    each(pa_wait)
    peaks[m] = jnp.max(pa[...], axis=0)

    def pb_copy(d):
        return rcopy(peaks.at[m], peaks.at[m], pb_s.at[d], pb_r.at[d], {"mp": mp_at(d)})

    def pb_wait(d):
        src = lax.rem(m + 16 - d, 16)
        rcopy(peaks.at[src], peaks.at[src], pb_s.at[d], pb_r.at[d], {"mp": src}).wait_recv()

    each(lambda d: pb_copy(d).start())
    each(lambda d: pa_copy(d).wait_send())
    each(pb_wait)
    each(lambda d: pb_copy(d).wait_send())


def outputs(made, width, logs, peaks, lower, newc, shift, lognorm, newlow):
    newc[...] = made[...]
    shift[...] = width[:, : shift.shape[1]]
    lognorm[...] = logs[...]
    for s in range(16):
        newlow[s : s + 1, :] = lower[s : s + 1, :] - jnp.concatenate([peaks[s]] * 4, axis=1)


def on_device(data_rows, centroids, block_mask, lower_bound):
    rows, feat = data_rows.shape
    blocks = rows // BLOCK
    width = centroids.shape[0]
    half = feat // 2
    own = width // 16
    items = 2 * (feat // 256)
    dma = pltpu.SemaphoreType.DMA
    vmem = pltpu.VMEM
    made, movement, log_norm, peaks = pl.pallas_call(
        kernel,
        name="kmeans_step",
        out_shape=(
            jax.ShapeDtypeStruct((own, feat), F32),
            jax.ShapeDtypeStruct((1, BLOCK), F32),
            jax.ShapeDtypeStruct((blocks, BLOCK), F32),
            jax.ShapeDtypeStruct((16, 1, BLOCK), F32),
        ),
        in_specs=[pl.BlockSpec(memory_space=pl.ANY)] * 3,
        out_specs=[pl.BlockSpec(memory_space=vmem)] * 4,
        scratch_shapes=[
            vmem((2, rows, half), BF16),
            vmem((2, width, feat), BF16),
            vmem((blocks, 16), jnp.int32),
            vmem((2, 2, rows, half), BF16),
            vmem((2, 2, 8 * BLOCK, half), BF16),
            vmem((3, 2, 2, BLOCK, half), BF16),
            vmem((2, 2, 2, BLOCK, half), BF16),
            vmem((8, 4, 4, own, 256), F32),
            vmem((2, width, 8 * BLOCK), BF16),
            vmem((8, 4, 4, own, 256), F32),
            vmem((items, 2, 2, own, 256), BF16),
            vmem((items, 2, 2, own, 256), BF16),
            vmem((items, 2, 4, own, 256), F32),
            vmem((items, 2, own // 2, 256), F32),
            vmem((items, 2, own, 256), F32),
            vmem((8, own, 256), F32),
            vmem((8, own, 256), F32),
            vmem((own, feat), F32),
            vmem((4, BLOCK), F32),
            vmem((16, 1, 16), F32),
            vmem((16, 8, 2, BLOCK), F32),
            vmem((16, 8, 2, BLOCK), F32),
            vmem((8, 2, BLOCK), F32),
            vmem((2, 8, 2, BLOCK), F32),
            vmem((2, width, BLOCK), F32),
            vmem((2, width, BLOCK), F32),
            vmem((16, 2, 1, width), F32),
            vmem((1, width), F32),
            vmem((1, width), F32),
            vmem((width, BLOCK), F32),
            vmem((16, 1, BLOCK), F32),
            dma((4,)),
            dma((16,)),
            dma((16,)),
            dma((1,)),
            dma((1,)),
            dma((16,)),
            dma((16,)),
            dma((2, 2)),
            dma((2, 2)),
            dma((3, 2, 2)),
            dma((3, 2, 2)),
            dma((2, 2, 2)),
            dma((2, 2, 2)),
            dma((2, 16)),
            dma((2, 16)),
            dma((16,)),
            dma((16,)),
            *[dma((items, 2)) for _ in range(8)],
            dma((8,)),
            dma((8,)),
            dma((1,)),
            dma((1,)),
            *[dma((16,)) for _ in range(4)],
        ],
        compiler_params=pltpu.CompilerParams(
            collective_id=0, has_side_effects=True, vmem_limit_bytes=66_000_000
        ),
    )(data_rows, centroids, block_mask.T)
    updated, movement, log_norm, new_lower = pl.pallas_call(
        outputs,
        name="outputs",
        out_shape=(
            jax.ShapeDtypeStruct(made.shape, F32),
            jax.ShapeDtypeStruct((1, own), F32),
            jax.ShapeDtypeStruct(log_norm.shape, F32),
            jax.ShapeDtypeStruct(lower_bound.shape, F32),
        ),
        in_specs=[pl.BlockSpec(memory_space=vmem)] * 5,
        out_specs=[pl.BlockSpec(memory_space=vmem)] * 4,
    )(made, movement, log_norm, peaks, lower_bound)
    return updated, movement.reshape(-1), log_norm.reshape(-1), new_lower


def solution(mesh):
    in_specs = (
        P(("dp", "mp"), None),
        P("mp", None),
        P(None, ("dp", "mp")),
        P(None, ("dp", "mp")),
    )
    out_specs = (
        P(("mp", "dp"), None),
        P(("mp", "dp")),
        P(("dp", "mp")),
        P(None, ("dp", "mp")),
    )
    return jax.shard_map(
        on_device, mesh=mesh, in_specs=in_specs, out_specs=out_specs, check_vma=False
    )
```

```python
import functools
import math

import jax
import jax.numpy as jnp
from jax import lax
from jax.experimental import pallas as pl
from jax.experimental.pallas import tpu as pltpu
from jax.sharding import PartitionSpec as P

BLOCK = 128
MESH = pl.DeviceIdType.MESH
NEG = -1e30
F32 = jnp.float32
BF16 = jnp.bfloat16


def rcopy(src, dst, ssem, rsem, dev):
    return pltpu.make_async_remote_copy(
        src_ref=src,
        dst_ref=dst,
        send_sem=ssem,
        recv_sem=rsem,
        device_id=dev,
        device_id_type=MESH,
    )


def kernel(
    data_in,
    cent_in,
    mask_in,
    newc,
    shift,
    lognorm,
    peaks,
    data,
    cent,
    mask,
    full,
    got,
    part,
    selb,
    sc,
    wt,
    sums,
    s1,
    r1,
    r2,
    r3,
    r4,
    te,
    re,
    rz,
    tot,
    cm,
    cv,
    ct,
    st,
    tops,
    nrm,
    cnorm,
    cacc,
    cbuf,
    csend,
    cret,
    ccol,
    pa,
    load_s,
    code_s,
    code_r,
    cs_s,
    cs_r,
    bc_s,
    bc_r,
    full_s,
    full_r,
    part_s,
    part_r,
    sel_s,
    sel_r,
    stat_s,
    stat_r,
    cnt_s,
    cnt_r,
    r1_s,
    r1_r,
    r2_s,
    r2_r,
    r3_s,
    r3_r,
    r4_s,
    r4_r,
    r5_s,
    r5_r,
    ret_s,
    ret_r,
    cret_s,
    cret_r,
    rz_s,
    rz_r,
    pa_s,
    pa_r,
    pb_s,
    pb_r,
):
    half = data.shape[2]
    feat = 2 * half
    width = cent.shape[1]
    own = width // 16
    sharp = 4.0 / math.sqrt(feat)
    p = lax.axis_index("dp")
    m = lax.axis_index("mp")
    z, c = m // 2, lax.rem(m, 2)
    y, x = p // 4, lax.rem(p, 4)
    sign = 1 - 2 * c
    step = (1, -1)
    reach = ((0, 1, -1, 2), (0, 1, -1, -2))
    mine_rows = pl.ds(pl.multiple_of(p * own, own), own)

    def chip(k):
        return lax.rem(z + sign * k + 16, 8)

    def lane(j):
        return c if j == 0 else 1 - c

    def lane_of(j):
        return pl.ds(lane(j), 1)

    def at(k, j):
        return chip(k) * 2 + lane(j)

    def dev(k, j):
        return {"mp": at(k, j)}

    def host(n, k, j):
        if n == 0:
            return at(k, j)
        return at(k + 3, 0) if j == 0 else at(k - 3, 1)

    def slot(n, h, pos, j):
        return got.at[n, h, (pos * 2 + j) * BLOCK : (pos * 2 + j + 1) * BLOCK, :]

    def mp_at(d):
        return lax.rem(m + d, 16)

    def dp_at(d):
        return lax.rem(p + d, 16)

    def each(body):
        lax.fori_loop(1, 16, lambda d, _: (body(d), _)[1], 0)

    barrier = pltpu.get_barrier_semaphore()

    def greet(d):
        pl.semaphore_signal(barrier, inc=1, device_id={"mp": mp_at(d)}, device_id_type=MESH)
        pl.semaphore_signal(barrier, inc=1, device_id={"dp": dp_at(d)}, device_id_type=MESH)

    loads = [pltpu.make_async_copy(mask_in, mask, load_s.at[0])]
    for h in range(2):
        src = data_in.at[:, h * half : (h + 1) * half]
        loads.append(pltpu.make_async_copy(src, data.at[h], load_s.at[1 + h]))
    loads.append(pltpu.make_async_copy(cent_in, cent.at[0], load_s.at[3]))
    for load in loads:
        load.start()
    each(greet)

    loads[0].wait()
    label = (lax.broadcasted_iota(jnp.int32, mask.shape, 0) + 1).astype(F32)
    code = jnp.sum(mask[...].astype(F32) * label, axis=0, keepdims=True)
    cv[m] = code
    shards = lax.broadcasted_iota(jnp.int32, code.shape, 1)
    for n in range(2):
        for j in range(2):
            here = jnp.where(shards == host(n, 0, j), code, 0.0)
            here = jnp.sum(here, axis=1, keepdims=True)
            cm[2 * n + j : 2 * n + j + 1, :] = jnp.broadcast_to(here, (1, BLOCK))
    for load in loads[1:]:
        load.wait()
    pl.semaphore_wait(barrier, 30)

    def code_copy(d):
        return rcopy(cv.at[m], cv.at[m], code_s.at[d], code_r.at[d], {"mp": mp_at(d)})

    def code_wait(d):
        src = lax.rem(m + 16 - d, 16)
        rcopy(cv.at[src], cv.at[src], code_s.at[d], code_r.at[d], {"mp": src}).wait_recv()

    slice_copy = rcopy(cent.at[0, mine_rows], cent.at[1, mine_rows], cs_s.at[0], cs_r.at[0], dev(-3, 0))

    def spread_copy(d):
        ref = cent.at[1, mine_rows]
        return rcopy(ref, ref, bc_s.at[d], bc_r.at[d], {"dp": dp_at(d)})

    def spread_wait(d):
        src = lax.rem(p + 16 - d, 16)
        ref = cent.at[1, pl.ds(pl.multiple_of(src * own, own), own)]
        rcopy(ref, ref, bc_s.at[d], bc_r.at[d], {"dp": src}).wait_recv()

    def full_copy(way, h):
        return rcopy(
            data.at[h], full.at[way, h], full_s.at[way, h], full_r.at[way, h], dev(step[way], 0)
        )

    each(lambda d: code_copy(d).start())
    slice_copy.start()
    for h in range(2):
        for way in range(2):
            full_copy(way, h).start()

    def choose(dst, src, code):
        code = jnp.broadcast_to(code, (BLOCK, BLOCK)).astype(BF16)
        for lanes in range(0, half, BLOCK):
            cols = slice(lanes, lanes + BLOCK)
            out = src[0:BLOCK, cols]
            for b in range(1, src.shape[0] // BLOCK):
                here = code == jnp.asarray(b + 1, BF16)
                out = jnp.where(here, src[b * BLOCK : (b + 1) * BLOCK, cols], out)
            dst[:, cols] = out

    def part_copy(i, n, h):
        return rcopy(
            part.at[i, n, h], slot(n, h, i, 1), part_s.at[i, n, h], part_r.at[i, n, h], dev(0, 1)
        )

    for n in range(2):
        for h in range(2):
            choose(part.at[0, n, h], data.at[h], cm[2 * n + 1 : 2 * n + 2, :])
            choose(slot(n, h, 0, 0), data.at[h], cm[2 * n : 2 * n + 1, :])
    for n in range(2):
        for h in range(2):
            part_copy(0, n, h).start()

    def norms_of(n):
        square = jnp.square(cent[n].astype(F32))
        square = jnp.sum(square, axis=1, keepdims=True)
        cnorm[n] = jnp.broadcast_to(square, cnorm.shape[1:])

    norms_of(0)

    each(code_wait)
    codes = cv[:, 0, :]
    for s in range(16):
        column = jnp.broadcast_to(codes[:, s : s + 1], (16, BLOCK))
        for zg in range(8):
            ct[s, zg] = column[2 * zg : 2 * zg + 2]

    slice_copy.wait_recv()
    each(lambda d: spread_copy(d).start())

    def code_of(k, j, shard):
        return ct[shard, chip(k), lane_of(j), :]

    def product(n, pos, h):
        return lax.dot_general(
            cent[n, :, h * half : (h + 1) * half],
            got[n, h, pos * 256 : (pos + 1) * 256, :],
            (((1,), (1,)), ((), ())),
            preferred_element_type=F32,
        )

    def weigh_up(n, pos, prod):
        score = sharp * (2.0 * prod - cnorm[n, :, 0:1])
        best = jnp.max(score, axis=0, keepdims=True)
        power = jnp.exp(score - best)
        sc[n * 4 + pos] = power.reshape(sc.shape[1:])
        whole = best + jnp.log(jnp.sum(power, axis=0, keepdims=True))
        row = pos * 2 + n
        for j in range(2):
            valid = code_of(reach[n][pos], j, host(n, 0, 0)) > 0.0
            lanes = slice(j * BLOCK, (j + 1) * BLOCK)
            tops[row, lane_of(j), :] = best[:, lanes]
            st[m, row, lane_of(j), :] = jnp.where(valid, whole[:, lanes], NEG)

    def scores(n, pos):
        weigh_up(n, pos, product(n, pos, 0) + product(n, pos, 1))

    def keep(way, h):
        k = -step[way]
        for n in range(2):
            choose(part.at[1 + way, n, h], full.at[way, h], code_of(k, 0, host(n, 0, 1)))
            choose(slot(n, h, 2 - way, 0), full.at[way, h], code_of(k, 0, host(n, 0, 0)))

    def sel_copy(way, j, h):
        n = 1 if way == j else 0
        return rcopy(
            selb.at[way, j, h],
            slot(n, h, 3, j),
            sel_s.at[way, j, h],
            sel_r.at[way, j, h],
            dev(step[way], j),
        )

    def select(way, j, h):
        n = 1 if way == j else 0
        code = code_of(-step[way], 0, host(n, step[way], j))
        choose(selb.at[way, j, h], full.at[way, h], code)

    for h in range(2):
        for way in range(2):
            full_copy(way, h).wait_recv()
            for j in range(2):
                select(way, j, h)
            keep(way, h)
            for j in (way, 1 - way)[: 2 - h]:
                sel_copy(way, j, h).start()
            for n in range(2):
                part_copy(1 + way, n, h).start()
        if h == 0:
            for hh in range(2):
                part_copy(0, 0, hh).wait_recv()
            scores(0, 0)
    for pos in (1, 2):
        for h in range(2):
            part_copy(pos, 0, h).wait_recv()
        scores(0, pos)
    each(spread_wait)
    norms_of(1)
    for pos in range(3):
        for h in range(2):
            part_copy(pos, 1, h).wait_recv()
        scores(1, pos)

    parts = (slice(0, 6), slice(6, 8))

    def stat_copy(n, d):
        ref = st.at[m, parts[n]]
        return rcopy(ref, ref, stat_s.at[n, d], stat_r.at[n, d], {"mp": mp_at(d)})

    def stat_wait(n, d):
        src = lax.rem(m + 16 - d, 16)
        ref = st.at[src, parts[n]]
        rcopy(ref, ref, stat_s.at[n, d], stat_r.at[n, d], {"mp": src}).wait_recv()

    each(lambda d: stat_copy(0, d).start())
    for way in range(2):
        sel_copy(way, 1 - way, 1).start()
    for h in range(2):
        for n in (1, 0):
            for way in range(2):
                sel_copy(way, way if n == 1 else 1 - way, h).wait_recv()
            prod = product(n, 3, h)
            if h == 0:
                sc[n * 4 + 3] = prod.reshape(sc.shape[1:])
            else:
                weigh_up(n, 3, sc[n * 4 + 3].reshape(width, 256) + prod)
    each(lambda d: stat_copy(1, d).start())
    each(lambda d: stat_wait(0, d))
    each(lambda d: stat_wait(1, d))

    def log_sum(pieces):
        top = functools.reduce(jnp.maximum, pieces)
        ceiling = jnp.maximum(top, 0.0)
        total = functools.reduce(jnp.add, [jnp.exp(piece - ceiling) for piece in pieces])
        return ceiling + jnp.log(jnp.exp(-ceiling) + total)

    near = {0: 0, 1: 1, 7: 2, 2: 3}
    afar = {0: 0, 1: 1, 7: 2, 6: 3}

    def scored(zg, s):
        q, turn = s // 2, 1 - 2 * (s % 2)
        d = (turn * (zg - q)) % 8
        if d in near:
            return s, near[d] * 2
        return ((q - 3 * turn) % 8) * 2 + s % 2, afar[(d + 3) % 8] * 2 + 1

    for zg in range(8):
        for n in range(2):
            mine = ct[host(n, 0, 0), zg]
            pieces = []
            for s in range(16):
                who, row = scored(zg, s)
                pieces.append(jnp.where(ct[s, zg] == mine, st[who, row], NEG))
            nrm[n, zg] = log_sum(pieces)

    def weigh(n):
        for pos in range(4):
            k = reach[n][pos]
            for j in range(2):
                cols = slice(j * BLOCK, (j + 1) * BLOCK)
                gap = tops[pos * 2 + n, lane_of(j), :] - nrm[n, chip(k), lane_of(j), :]
                scale = jnp.where(code_of(k, j, host(n, 0, 0)) > 0.0, jnp.exp(gap), 0.0)
                power = sc[n * 4 + pos, :, :, :, cols].reshape(width, BLOCK)
                weight = power * scale
                if pos == 0 and j == 0:
                    cacc[n] = weight
                else:
                    cacc[n] += weight
                wt[n, :, pos * 256 + j * BLOCK : pos * 256 + (j + 1) * BLOCK] = weight.astype(BF16)

    weigh(1)

    each_set = 2 * (half // 256)
    items = 2 * each_set
    held = (sc, sums)
    first = (x, y)
    second = (y, x)

    def dp_dev(a, b):
        return {"dp": lax.rem(y + a + 4, 4) * 4 + lax.rem(x + b + 4, 4)}

    def first_dev(h, d):
        return dp_dev(0, d) if h == 0 else dp_dev(d, 0)

    def second_dev(h, d):
        return dp_dev(d, 0) if h == 0 else dp_dev(0, d)

    def plus(v, d):
        return lax.rem(v + d + 4, 4)

    last_q = half // 256 - 1

    def item(n):
        i = n % each_set
        h, q = i % 2, i // 2
        if n < each_set:
            q = (q + last_q) % (last_q + 1)
        return (1 if n < each_set else 0), 2 * q + h, h, q

    def half_rows(way):
        return pl.ds(way * (own // 2), own // 2)

    def wide(n):
        return pl.ds(0, BLOCK if n < 2 else 256)

    def direct(n):
        return n >= items - 2

    def copy1(n, way):
        h, cols = item(n)[2], wide(n)
        src, dst = s1.at[n, way, :, :, cols], r1.at[n, way, :, :, cols]
        return rcopy(src, dst, r1_s.at[n, way], r1_r.at[n, way], first_dev(h, step[way]))

    def copy2(n, way, late):
        (e, i, h, q), cols = item(n), wide(n)
        some = slice(0, 2) if late == (way == 0) else slice(2, 4)
        src = held[e].at[i, plus(first[h], step[way]), some, :, cols]
        dst = r2.at[n, way, some, :, cols]
        sems = (r2_s, r2_r) if late else (r5_s, r5_r)
        return rcopy(src, dst, sems[0].at[n, way], sems[1].at[n, way], first_dev(h, step[way]))

    def copy3(n, way):
        (e, i, h, q), cols = item(n), wide(n)
        src = held[e].at[i, first[h], plus(second[h], 2), half_rows(way), cols]
        dst = r3.at[n, way, :, cols]
        hops = 2 if direct(n) else step[way]
        return rcopy(src, dst, r3_s.at[n, way], r3_r.at[n, way], second_dev(h, hops))

    def copy4(n, way):
        (e, i, h, q), cols = item(n), wide(n)
        src = held[e].at[i, first[h], plus(second[h], step[way]), :, cols]
        dst = r4.at[n, way, :, cols]
        return rcopy(src, dst, r4_s.at[n, way], r4_r.at[n, way], second_dev(h, step[way]))

    def back_copy(i):
        cols = wide(0 if i // 2 == last_q else items)
        src, dst = te.at[i, :, cols], re.at[i, :, cols]
        return rcopy(src, dst, ret_s.at[i], ret_r.at[i], dev(3, 0))

    def home_copy(h):
        src = sums.at[2 * last_q + h, :, :, :, BLOCK:256]
        return rcopy(src, rz.at[h], rz_s.at[h], rz_r.at[h], dev(3, 0))

    def stage1(n):
        e, i, h, q = item(n)
        out = jnp.dot(wt[e], got[e, h, :, q * 256 : (q + 1) * 256], preferred_element_type=F32)
        for owner in range(16):
            yy, xx = owner // 4, owner % 4
            a, b = (xx, yy) if h == 0 else (yy, xx)
            held[e][i, a, b] = out[owner * own : (owner + 1) * own]
        if n >= items - 2:
            home_copy(h).wait_recv()
            held[e][i, :, :, :, BLOCK:256] += rz[h]
        for way in range(2):
            s1[n, way] = held[e][i, plus(first[h], 2), 2 * way : 2 * way + 2].astype(BF16)
        for way in range(2):
            copy1(n, way).start()
        for way in range(2):
            copy2(n, way, False).start()
        if n < 2:
            home_copy(h).start()

    def stage2(n):
        (e, i, h, q), cols = item(n), wide(n)
        for way in range(2):
            copy1(n, way).wait_recv()
            a = plus(first[h], step[way])
            held[e][i, a, 2 * way : 2 * way + 2, :, cols] += r1[n, way, :, :, cols].astype(F32)
            copy2(n, way, True).start()

    def stage3(n):
        (e, i, h, q), cols = item(n), wide(n)
        for way in range(2):
            copy2(n, way, False).wait_recv()
            copy2(n, way, True).wait_recv()
        held[e][i, first[h], :, :, cols] += r2[n, 0, :, :, cols] + r2[n, 1, :, :, cols]
        for way in range(2):
            copy3(n, way).start()
        if direct(n):
            for way in range(2):
                copy4(n, way).start()

    def stage4(n):
        if direct(n):
            return
        (e, i, h, q), cols = item(n), wide(n)
        for way in range(2):
            copy3(n, way).wait_recv()
            b = plus(second[h], step[way])
            held[e][i, first[h], b, half_rows(way), cols] += r3[n, way, :, cols]
            copy4(n, way).start()

    def finish(n):
        (e, i, h, q), cols = item(n), wide(n)
        for way in range(2):
            copy4(n, way).wait_recv()
            if direct(n):
                copy3(n, way).wait_recv()
        value = held[e][i, first[h], second[h], :, cols] + r4[n, 0, :, cols] + r4[n, 1, :, cols]
        if direct(n):
            value = value + jnp.concatenate([r3[n, 0], r3[n, 1]], axis=0)
        if e == 1:
            te[i, :, cols] = value
            back_copy(i).start()
        else:
            back_copy(i).wait_recv()
            start = h * half + q * 256
            tot[:, start : start + 256] = value
            had = BLOCK if q == last_q else 256
            tot[:, start : start + had] += re[i, :, :had]

    def cnt_copy(d):
        return rcopy(cbuf.at[p], cbuf.at[p], cnt_s.at[d], cnt_r.at[d], {"dp": dp_at(d)})

    def cnt_wait(d):
        src = lax.rem(p + 16 - d, 16)
        rcopy(cbuf.at[src], cbuf.at[src], cnt_s.at[d], cnt_r.at[d], {"dp": src}).wait_recv()

    count_back = rcopy(csend, cret, cret_s.at[0], cret_r.at[0], dev(3, 0))

    stages = ((stage1, 0), (stage2, 3), (stage3, 8), (stage4, 13), (finish, 18))
    for t in range(items + 18):
        for stage, late in stages:
            if 0 <= t - late < items:
                stage(t - late)
        if t == 3:
            weigh(0)
            for n in range(2):
                cbuf[p, n] = jnp.sum(cacc[n].T, axis=0, keepdims=True)
            each(lambda d: cnt_copy(d).start())
        if t == items - 1:
            each(cnt_wait)
            csend[...] = jnp.sum(cbuf[:, 1], axis=0)
            count_back.start()
            number = (lax.broadcasted_iota(jnp.int32, (4, BLOCK), 0) + 1).astype(F32)
            pieces = []
            for s in range(16):
                q, turn = s // 2, 1 - 2 * (s % 2)
                d = lax.rem(turn * (z - q) + 16, 8)
                at_home = (d <= 2) | (d == 7)
                who = jnp.where(at_home, s, lax.rem(q - 3 * turn + 8, 8) * 2 + s % 2)
                d = jnp.where(at_home, d, lax.rem(d + 3, 8))
                pos = jnp.where(d == 0, 0, jnp.where(d == 1, 1, jnp.where(d == 7, 2, 3)))
                row = pos * 2 + jnp.where(at_home, 0, 1)
                here = ct[s, z, lane_of(0), :] == number
                pieces.append(jnp.where(here, st[who, row, lane_of(0), :], NEG))
            lognorm[...] = log_sum(pieces)
        if t == items + 4:
            count_back.wait_recv()
            count = jnp.sum(cbuf[:, 0], axis=0) + cret[...]
            ccol[...] = jnp.broadcast_to(count, (BLOCK, width)).T

    old = cent[0, mine_rows, :].astype(F32)
    denom = ccol[mine_rows, 0:1] + 1.0
    updated = (tot[...] + old) / denom
    newc[...] = updated
    move = jnp.sqrt(jnp.sum(jnp.square(updated - old), axis=1, keepdims=True) + 1.0)
    moves = jnp.broadcast_to(move, (own, BLOCK))
    pa[p] = jnp.max(moves, axis=0, keepdims=True)

    def pa_copy(d):
        return rcopy(pa.at[p], pa.at[p], pa_s.at[d], pa_r.at[d], {"dp": dp_at(d)})

    def pa_wait(d):
        src = lax.rem(p + 16 - d, 16)
        rcopy(pa.at[src], pa.at[src], pa_s.at[d], pa_r.at[d], {"dp": src}).wait_recv()

    each(lambda d: pa_copy(d).start())
    tall = jnp.concatenate([moves, jnp.zeros((BLOCK - own, BLOCK), F32)], axis=0)
    shift[...] = tall.T[0:1, :]

    slice_copy.wait_send()
    count_back.wait_send()
    for h in range(2):
        for way in range(2):
            full_copy(way, h).wait_send()
            for j in range(2):
                sel_copy(way, j, h).wait_send()
        for n in range(2):
            for i in range(3):
                part_copy(i, n, h).wait_send()
    for n in range(items):
        for way in range(2):
            for copy in (copy1, copy3, copy4):
                copy(n, way).wait_send()
            for late in (False, True):
                copy2(n, way, late).wait_send()
    for i in range(each_set):
        back_copy(i).wait_send()
    for h in range(2):
        home_copy(h).wait_send()

    def sent(d):
        for copy in (code_copy, spread_copy, cnt_copy):
            copy(d).wait_send()
        for n in range(2):
            stat_copy(n, d).wait_send()

    each(sent)

    each(pa_wait)
    peaks[m] = jnp.max(pa[...], axis=0)

    def pb_copy(d):
        return rcopy(peaks.at[m], peaks.at[m], pb_s.at[d], pb_r.at[d], {"mp": mp_at(d)})

    def pb_wait(d):
        src = lax.rem(m + 16 - d, 16)
        rcopy(peaks.at[src], peaks.at[src], pb_s.at[d], pb_r.at[d], {"mp": src}).wait_recv()

    each(lambda d: pb_copy(d).start())
    each(lambda d: pa_copy(d).wait_send())
    each(pb_wait)
    each(lambda d: pb_copy(d).wait_send())


def outputs(made, width, logs, peaks, lower, newc, shift, lognorm, newlow):
    newc[...] = made[...]
    shift[...] = width[:, : shift.shape[1]]
    lognorm[...] = logs[...]
    for s in range(16):
        newlow[s : s + 1, :] = lower[s : s + 1, :] - jnp.concatenate([peaks[s]] * 4, axis=1)


def on_device(data_rows, centroids, block_mask, lower_bound):
    rows, feat = data_rows.shape
    blocks = rows // BLOCK
    width = centroids.shape[0]
    half = feat // 2
    own = width // 16
    items = 2 * (feat // 256)
    dma = pltpu.SemaphoreType.DMA
    vmem = pltpu.VMEM
    made, movement, log_norm, peaks = pl.pallas_call(
        kernel,
        name="kmeans_step",
        out_shape=(
            jax.ShapeDtypeStruct((own, feat), F32),
            jax.ShapeDtypeStruct((1, BLOCK), F32),
            jax.ShapeDtypeStruct((blocks, BLOCK), F32),
            jax.ShapeDtypeStruct((16, 1, BLOCK), F32),
        ),
        in_specs=[pl.BlockSpec(memory_space=pl.ANY)] * 3,
        out_specs=[pl.BlockSpec(memory_space=vmem)] * 4,
        scratch_shapes=[
            vmem((2, rows, half), BF16),
            vmem((2, width, feat), BF16),
            vmem((blocks, 16), jnp.int32),
            vmem((2, 2, rows, half), BF16),
            vmem((2, 2, 8 * BLOCK, half), BF16),
            vmem((3, 2, 2, BLOCK, half), BF16),
            vmem((2, 2, 2, BLOCK, half), BF16),
            vmem((8, 4, 4, own, 256), F32),
            vmem((2, width, 8 * BLOCK), BF16),
            vmem((8, 4, 4, own, 256), F32),
            vmem((items, 2, 2, own, 256), BF16),
            vmem((items, 2, 2, own, 256), BF16),
            vmem((items, 2, 4, own, 256), F32),
            vmem((items, 2, own // 2, 256), F32),
            vmem((items, 2, own, 256), F32),
            vmem((8, own, 256), F32),
            vmem((8, own, 256), F32),
            vmem((2, 4, 4, own, BLOCK), F32),
            vmem((own, feat), F32),
            vmem((4, BLOCK), F32),
            vmem((16, 1, 16), F32),
            vmem((16, 8, 2, BLOCK), F32),
            vmem((16, 8, 2, BLOCK), F32),
            vmem((8, 2, BLOCK), F32),
            vmem((2, 8, 2, BLOCK), F32),
            vmem((2, width, BLOCK), F32),
            vmem((2, width, BLOCK), F32),
            vmem((16, 2, 1, width), F32),
            vmem((1, width), F32),
            vmem((1, width), F32),
            vmem((width, BLOCK), F32),
            vmem((16, 1, BLOCK), F32),
            dma((4,)),
            dma((16,)),
            dma((16,)),
            dma((1,)),
            dma((1,)),
            dma((16,)),
            dma((16,)),
            dma((2, 2)),
            dma((2, 2)),
            dma((3, 2, 2)),
            dma((3, 2, 2)),
            dma((2, 2, 2)),
            dma((2, 2, 2)),
            dma((2, 16)),
            dma((2, 16)),
            dma((16,)),
            dma((16,)),
            *[dma((items, 2)) for _ in range(10)],
            dma((8,)),
            dma((8,)),
            dma((1,)),
            dma((1,)),
            dma((2,)),
            dma((2,)),
            *[dma((16,)) for _ in range(4)],
        ],
        compiler_params=pltpu.CompilerParams(
            collective_id=0, has_side_effects=True, vmem_limit_bytes=66_000_000
        ),
    )(data_rows, centroids, block_mask.T)
    updated, movement, log_norm, new_lower = pl.pallas_call(
        outputs,
        name="outputs",
        out_shape=(
            jax.ShapeDtypeStruct(made.shape, F32),
            jax.ShapeDtypeStruct((1, own), F32),
            jax.ShapeDtypeStruct(log_norm.shape, F32),
            jax.ShapeDtypeStruct(lower_bound.shape, F32),
        ),
        in_specs=[pl.BlockSpec(memory_space=vmem)] * 5,
        out_specs=[pl.BlockSpec(memory_space=vmem)] * 4,
    )(made, movement, log_norm, peaks, lower_bound)
    return updated, movement.reshape(-1), log_norm.reshape(-1), new_lower


def solution(mesh):
    in_specs = (
        P(("dp", "mp"), None),
        P("mp", None),
        P(None, ("dp", "mp")),
        P(None, ("dp", "mp")),
    )
    out_specs = (
        P(("mp", "dp"), None),
        P(("mp", "dp")),
        P(("dp", "mp")),
        P(None, ("dp", "mp")),
    )
    return jax.shard_map(
        on_device, mesh=mesh, in_specs=in_specs, out_specs=out_specs, check_vma=False
    )
```

```python
import functools
import math

import jax
import jax.numpy as jnp
from jax import lax
from jax.experimental import pallas as pl
from jax.experimental.pallas import tpu as pltpu
from jax.sharding import PartitionSpec as P

BLOCK = 128
MESH = pl.DeviceIdType.MESH
NEG = -1e30
F32 = jnp.float32
BF16 = jnp.bfloat16


def rcopy(src, dst, ssem, rsem, dev):
    return pltpu.make_async_remote_copy(
        src_ref=src,
        dst_ref=dst,
        send_sem=ssem,
        recv_sem=rsem,
        device_id=dev,
        device_id_type=MESH,
    )


def kernel(
    data_in,
    cent_in,
    mask_in,
    newc,
    shift,
    lognorm,
    peaks,
    data,
    cent,
    mask,
    full,
    got,
    part,
    selb,
    sc,
    wt,
    sums,
    s1,
    r1,
    r2,
    r3,
    r4,
    te,
    re,
    rz,
    tot,
    cm,
    cv,
    ct,
    st,
    tops,
    nrm,
    cnorm,
    cacc,
    cbuf,
    csend,
    cret,
    ccol,
    pa,
    load_s,
    code_s,
    code_r,
    cs_s,
    cs_r,
    bc_s,
    bc_r,
    full_s,
    full_r,
    part_s,
    part_r,
    sel_s,
    sel_r,
    stat_s,
    stat_r,
    cnt_s,
    cnt_r,
    r1_s,
    r1_r,
    r2_s,
    r2_r,
    r3_s,
    r3_r,
    r4_s,
    r4_r,
    r5_s,
    r5_r,
    ret_s,
    ret_r,
    cret_s,
    cret_r,
    rz_s,
    rz_r,
    pa_s,
    pa_r,
    pb_s,
    pb_r,
):
    half = data.shape[2]
    feat = 2 * half
    width = cent.shape[1]
    own = width // 16
    sharp = 4.0 / math.sqrt(feat)
    p = lax.axis_index("dp")
    m = lax.axis_index("mp")
    z, c = m // 2, lax.rem(m, 2)
    y, x = p // 4, lax.rem(p, 4)
    sign = 1 - 2 * c
    step = (1, -1)
    reach = ((0, 1, -1, 2), (0, 1, -1, -2))
    mine_rows = pl.ds(pl.multiple_of(p * own, own), own)

    def chip(k):
        return lax.rem(z + sign * k + 16, 8)

    def lane(j):
        return c if j == 0 else 1 - c

    def lane_of(j):
        return pl.ds(lane(j), 1)

    def at(k, j):
        return chip(k) * 2 + lane(j)

    def dev(k, j):
        return {"mp": at(k, j)}

    def host(n, k, j):
        if n == 0:
            return at(k, j)
        return at(k + 3, 0) if j == 0 else at(k - 3, 1)

    def slot(n, h, pos, j):
        return got.at[n, h, (pos * 2 + j) * BLOCK : (pos * 2 + j + 1) * BLOCK, :]

    def mp_at(d):
        return lax.rem(m + d, 16)

    def dp_at(d):
        return lax.rem(p + d, 16)

    def each(body):
        lax.fori_loop(1, 16, lambda d, _: (body(d), _)[1], 0)

    barrier = pltpu.get_barrier_semaphore()

    def greet(d):
        pl.semaphore_signal(barrier, inc=1, device_id={"mp": mp_at(d)}, device_id_type=MESH)
        pl.semaphore_signal(barrier, inc=1, device_id={"dp": dp_at(d)}, device_id_type=MESH)

    loads = [pltpu.make_async_copy(mask_in, mask, load_s.at[0])]
    for h in range(2):
        src = data_in.at[:, h * half : (h + 1) * half]
        loads.append(pltpu.make_async_copy(src, data.at[h], load_s.at[1 + h]))
    loads.append(pltpu.make_async_copy(cent_in, cent.at[0], load_s.at[3]))
    for load in loads:
        load.start()
    each(greet)

    loads[0].wait()
    label = (lax.broadcasted_iota(jnp.int32, mask.shape, 0) + 1).astype(F32)
    code = jnp.sum(mask[...].astype(F32) * label, axis=0, keepdims=True)
    cv[m] = code
    shards = lax.broadcasted_iota(jnp.int32, code.shape, 1)
    for n in range(2):
        for j in range(2):
            here = jnp.where(shards == host(n, 0, j), code, 0.0)
            here = jnp.sum(here, axis=1, keepdims=True)
            cm[2 * n + j : 2 * n + j + 1, :] = jnp.broadcast_to(here, (1, BLOCK))
    for load in loads[1:]:
        load.wait()
    pl.semaphore_wait(barrier, 30)

    def code_copy(d):
        return rcopy(cv.at[m], cv.at[m], code_s.at[d], code_r.at[d], {"mp": mp_at(d)})

    def code_wait(d):
        src = lax.rem(m + 16 - d, 16)
        rcopy(cv.at[src], cv.at[src], code_s.at[d], code_r.at[d], {"mp": src}).wait_recv()

    slice_copy = rcopy(cent.at[0, mine_rows], cent.at[1, mine_rows], cs_s.at[0], cs_r.at[0], dev(-3, 0))

    def spread_copy(d):
        ref = cent.at[1, mine_rows]
        return rcopy(ref, ref, bc_s.at[d], bc_r.at[d], {"dp": dp_at(d)})

    def spread_wait(d):
        src = lax.rem(p + 16 - d, 16)
        ref = cent.at[1, pl.ds(pl.multiple_of(src * own, own), own)]
        rcopy(ref, ref, bc_s.at[d], bc_r.at[d], {"dp": src}).wait_recv()

    def full_copy(way, h):
        return rcopy(
            data.at[h], full.at[way, h], full_s.at[way, h], full_r.at[way, h], dev(step[way], 0)
        )

    each(lambda d: code_copy(d).start())
    slice_copy.start()
    for h in range(2):
        for way in range(2):
            full_copy(way, h).start()

    def choose(dst, src, code):
        code = jnp.broadcast_to(code, (BLOCK, BLOCK)).astype(BF16)
        for lanes in range(0, half, BLOCK):
            cols = slice(lanes, lanes + BLOCK)
            out = src[0:BLOCK, cols]
            for b in range(1, src.shape[0] // BLOCK):
                here = code == jnp.asarray(b + 1, BF16)
                out = jnp.where(here, src[b * BLOCK : (b + 1) * BLOCK, cols], out)
            dst[:, cols] = out

    def part_copy(i, n, h):
        return rcopy(
            part.at[i, n, h], slot(n, h, i, 1), part_s.at[i, n, h], part_r.at[i, n, h], dev(0, 1)
        )

    for n in range(2):
        for h in range(2):
            choose(part.at[0, n, h], data.at[h], cm[2 * n + 1 : 2 * n + 2, :])
            choose(slot(n, h, 0, 0), data.at[h], cm[2 * n : 2 * n + 1, :])
    for n in range(2):
        for h in range(2):
            part_copy(0, n, h).start()

    def norms_of(n):
        square = jnp.square(cent[n].astype(F32))
        square = jnp.sum(square, axis=1, keepdims=True)
        cnorm[n] = jnp.broadcast_to(square, cnorm.shape[1:])

    norms_of(0)

    each(code_wait)
    codes = cv[:, 0, :]
    for s in range(16):
        column = jnp.broadcast_to(codes[:, s : s + 1], (16, BLOCK))
        for zg in range(8):
            ct[s, zg] = column[2 * zg : 2 * zg + 2]

    slice_copy.wait_recv()
    each(lambda d: spread_copy(d).start())

    def code_of(k, j, shard):
        return ct[shard, chip(k), lane_of(j), :]

    def row_of(pos, n):
        return (1, 0, 2, 3)[pos] * 2 + n

    def product(n, pos, h):
        return lax.dot_general(
            cent[n, :, h * half : (h + 1) * half],
            got[n, h, pos * 256 : (pos + 1) * 256, :],
            (((1,), (1,)), ((), ())),
            preferred_element_type=F32,
        )

    def weigh_up(n, pos, prod):
        score = sharp * (2.0 * prod - cnorm[n, :, 0:1])
        best = jnp.max(score, axis=0, keepdims=True)
        power = jnp.exp(score - best)
        sc[n * 4 + pos] = power.reshape(sc.shape[1:])
        whole = best + jnp.log(jnp.sum(power, axis=0, keepdims=True))
        row = row_of(pos, n)
        for j in range(2):
            valid = code_of(reach[n][pos], j, host(n, 0, 0)) > 0.0
            lanes = slice(j * BLOCK, (j + 1) * BLOCK)
            tops[row, lane_of(j), :] = best[:, lanes]
            st[m, row, lane_of(j), :] = jnp.where(valid, whole[:, lanes], NEG)

    def scores(n, pos):
        weigh_up(n, pos, product(n, pos, 0) + product(n, pos, 1))

    def keep(way, h):
        k = -step[way]
        for n in range(2):
            choose(part.at[1 + way, n, h], full.at[way, h], code_of(k, 0, host(n, 0, 1)))
            choose(slot(n, h, 2 - way, 0), full.at[way, h], code_of(k, 0, host(n, 0, 0)))

    def sel_copy(way, j, h):
        n = 1 if way == j else 0
        return rcopy(
            selb.at[way, j, h],
            slot(n, h, 3, j),
            sel_s.at[way, j, h],
            sel_r.at[way, j, h],
            dev(step[way], j),
        )

    def select(way, j, h):
        n = 1 if way == j else 0
        code = code_of(-step[way], 0, host(n, step[way], j))
        choose(selb.at[way, j, h], full.at[way, h], code)

    for h in range(2):
        for way in range(2):
            full_copy(way, h).wait_recv()
            for j in range(2):
                select(way, j, h)
            keep(way, h)
            for j in (way, 1 - way)[: 2 - h]:
                sel_copy(way, j, h).start()
            for n in range(2):
                part_copy(1 + way, n, h).start()
        if h == 0:
            for hh in range(2):
                part_copy(0, 0, hh).wait_recv()
            scores(0, 0)
    for pos in (1, 2):
        for h in range(2):
            part_copy(pos, 0, h).wait_recv()
        scores(0, pos)
    each(spread_wait)
    norms_of(1)
    for pos in range(3):
        for h in range(2):
            part_copy(pos, 1, h).wait_recv()
        scores(1, pos)

    early = {0: (0, 6), 1: (0, 6), -1: (0, 6), 2: (0, 4), -2: (2, 6), 3: (0, 2), -3: (4, 6)}
    final = {k: (6 if k >= 0 else 7, 7 if 0 < k < 4 else 8) for k in range(-3, 5)}
    peers = [(k, j) for k in range(-3, 5) for j in range(2) if (k, j) != (0, 0)]

    def stat_copy(n, k, j, came):
        rows = (early, final)[n][k]
        src = m if not came else at(-k, 0) if j == 0 else at(k, 1)
        ref, i = st.at[src, rows[0] : rows[1]], (k + 3) * 2 + j
        return rcopy(ref, ref, stat_s.at[n, i], stat_r.at[n, i], {"mp": src} if came else dev(k, j))

    def stats(n):
        return [(n, k, j) for k, j in peers if n == 1 or k < 4]

    for one in stats(0):
        stat_copy(*one, False).start()
    for way in range(2):
        sel_copy(way, 1 - way, 1).start()
    for h in range(2):
        for n in (1, 0):
            for way in range(2):
                sel_copy(way, way if n == 1 else 1 - way, h).wait_recv()
            prod = product(n, 3, h)
            if h == 0:
                sc[n * 4 + 3] = prod.reshape(sc.shape[1:])
            else:
                weigh_up(n, 3, sc[n * 4 + 3].reshape(width, 256) + prod)
    for one in stats(1):
        stat_copy(*one, False).start()
    for one in stats(0) + stats(1):
        stat_copy(*one, True).wait_recv()

    def log_sum(pieces):
        top = functools.reduce(jnp.maximum, pieces)
        ceiling = jnp.maximum(top, 0.0)
        total = functools.reduce(jnp.add, [jnp.exp(piece - ceiling) for piece in pieces])
        return ceiling + jnp.log(jnp.exp(-ceiling) + total)

    near = {0: 0, 1: 1, 7: 2, 2: 3}
    afar = {0: 0, 1: 1, 7: 2, 6: 3}

    def log_sums(k, mine, lanes):
        pieces = []
        for q in range(-3, 5):
            for j in range(2):
                turn = 1 - 2 * j
                d = turn * (k - q) % 8
                who, row = at(q, j), 0
                if d in near:
                    row = row_of(near[d], 0)
                else:
                    who, row = at(q - 3 * turn, j), row_of(afar[(d + 3) % 8], 1)
                here = ct[at(q, j), chip(k), lanes, :] == mine
                pieces.append(jnp.where(here, st[who, row, lanes, :], NEG))
        return log_sum(pieces)

    for n in range(2):
        for pos in range(4):
            k = reach[n][pos]
            nrm[n, pos] = log_sums(k, ct[host(n, 0, 0), chip(k)], slice(0, 2))

    def weigh(n):
        for pos in range(4):
            k = reach[n][pos]
            for j in range(2):
                cols = slice(j * BLOCK, (j + 1) * BLOCK)
                gap = tops[row_of(pos, n), lane_of(j), :] - nrm[n, pos, lane_of(j), :]
                scale = jnp.where(code_of(k, j, host(n, 0, 0)) > 0.0, jnp.exp(gap), 0.0)
                power = sc[n * 4 + pos, :, :, :, cols].reshape(width, BLOCK)
                weight = power * scale
                if pos == 0 and j == 0:
                    cacc[n] = weight
                else:
                    cacc[n] += weight
                wt[n, :, pos * 256 + j * BLOCK : pos * 256 + (j + 1) * BLOCK] = weight.astype(BF16)

    weigh(1)

    each_set = 2 * (half // 256)
    items = 2 * each_set
    held = (sc, sums)
    first = (x, y)
    second = (y, x)

    def dp_dev(a, b):
        return {"dp": lax.rem(y + a + 4, 4) * 4 + lax.rem(x + b + 4, 4)}

    def first_dev(h, d):
        return dp_dev(0, d) if h == 0 else dp_dev(d, 0)

    def second_dev(h, d):
        return dp_dev(d, 0) if h == 0 else dp_dev(0, d)

    def plus(v, d):
        return lax.rem(v + d + 4, 4)

    last_q = half // 256 - 1

    def item(n):
        i = n % each_set
        h, q = i % 2, i // 2
        if n < each_set:
            q = (q + last_q) % (last_q + 1)
        return (1 if n < each_set else 0), 2 * q + h, h, q

    def half_rows(way):
        return pl.ds(way * (own // 2), own // 2)

    def wide(n):
        return pl.ds(0, BLOCK if n < 2 else 256)

    def direct(n):
        return n >= items - 2

    def copy1(n, way):
        h, cols = item(n)[2], wide(n)
        src, dst = s1.at[n, way, :, :, cols], r1.at[n, way, :, :, cols]
        return rcopy(src, dst, r1_s.at[n, way], r1_r.at[n, way], first_dev(h, step[way]))

    def copy2(n, way, late):
        (e, i, h, q), cols = item(n), wide(n)
        some = slice(0, 2) if late == (way == 0) else slice(2, 4)
        src = held[e].at[i, plus(first[h], step[way]), some, :, cols]
        dst = r2.at[n, way, some, :, cols]
        sems = (r2_s, r2_r) if late else (r5_s, r5_r)
        return rcopy(src, dst, sems[0].at[n, way], sems[1].at[n, way], first_dev(h, step[way]))

    def copy3(n, way):
        (e, i, h, q), cols = item(n), wide(n)
        src = held[e].at[i, first[h], plus(second[h], 2), half_rows(way), cols]
        dst = r3.at[n, way, :, cols]
        hops = 2 if direct(n) else step[way]
        return rcopy(src, dst, r3_s.at[n, way], r3_r.at[n, way], second_dev(h, hops))

    def copy4(n, way):
        (e, i, h, q), cols = item(n), wide(n)
        src = held[e].at[i, first[h], plus(second[h], step[way]), :, cols]
        dst = r4.at[n, way, :, cols]
        return rcopy(src, dst, r4_s.at[n, way], r4_r.at[n, way], second_dev(h, step[way]))

    def back_copy(i):
        cols = wide(0 if i // 2 == last_q else items)
        src, dst = te.at[i, :, cols], re.at[i, :, cols]
        return rcopy(src, dst, ret_s.at[i], ret_r.at[i], dev(3, 0))

    def home_copy(h):
        src = sums.at[2 * last_q + h, :, :, :, BLOCK:256]
        return rcopy(src, rz.at[h], rz_s.at[h], rz_r.at[h], dev(3, 0))

    def stage1(n):
        e, i, h, q = item(n)
        out = jnp.dot(wt[e], got[e, h, :, q * 256 : (q + 1) * 256], preferred_element_type=F32)
        for owner in range(16):
            yy, xx = owner // 4, owner % 4
            a, b = (xx, yy) if h == 0 else (yy, xx)
            held[e][i, a, b] = out[owner * own : (owner + 1) * own]
        if n >= items - 2:
            home_copy(h).wait_recv()
            held[e][i, :, :, :, BLOCK:256] += rz[h]
        for way in range(2):
            s1[n, way] = held[e][i, plus(first[h], 2), 2 * way : 2 * way + 2].astype(BF16)
        for way in range(2):
            copy1(n, way).start()
        for way in range(2):
            copy2(n, way, False).start()
        if n < 2:
            home_copy(h).start()

    def stage2(n):
        (e, i, h, q), cols = item(n), wide(n)
        for way in range(2):
            copy1(n, way).wait_recv()
            a = plus(first[h], step[way])
            held[e][i, a, 2 * way : 2 * way + 2, :, cols] += r1[n, way, :, :, cols].astype(F32)
            copy2(n, way, True).start()

    def stage3(n):
        (e, i, h, q), cols = item(n), wide(n)
        for way in range(2):
            copy2(n, way, False).wait_recv()
            copy2(n, way, True).wait_recv()
        held[e][i, first[h], :, :, cols] += r2[n, 0, :, :, cols] + r2[n, 1, :, :, cols]
        for way in range(2):
            copy3(n, way).start()
        if direct(n):
            for way in range(2):
                copy4(n, way).start()

    def stage4(n):
        if direct(n):
            return
        (e, i, h, q), cols = item(n), wide(n)
        for way in range(2):
            copy3(n, way).wait_recv()
            b = plus(second[h], step[way])
            held[e][i, first[h], b, half_rows(way), cols] += r3[n, way, :, cols]
            copy4(n, way).start()

    def finish(n):
        (e, i, h, q), cols = item(n), wide(n)
        for way in range(2):
            copy4(n, way).wait_recv()
            if direct(n):
                copy3(n, way).wait_recv()
        value = held[e][i, first[h], second[h], :, cols] + r4[n, 0, :, cols] + r4[n, 1, :, cols]
        if direct(n):
            value = value + jnp.concatenate([r3[n, 0], r3[n, 1]], axis=0)
        if e == 1:
            te[i, :, cols] = value
            back_copy(i).start()
        else:
            back_copy(i).wait_recv()
            start = h * half + q * 256
            tot[:, start : start + 256] = value
            had = BLOCK if q == last_q else 256
            tot[:, start : start + had] += re[i, :, :had]

    def cnt_copy(d):
        return rcopy(cbuf.at[p], cbuf.at[p], cnt_s.at[d], cnt_r.at[d], {"dp": dp_at(d)})

    def cnt_wait(d):
        src = lax.rem(p + 16 - d, 16)
        rcopy(cbuf.at[src], cbuf.at[src], cnt_s.at[d], cnt_r.at[d], {"dp": src}).wait_recv()

    count_back = rcopy(csend, cret, cret_s.at[0], cret_r.at[0], dev(3, 0))

    stages = ((stage1, 0), (stage2, 4), (stage3, 8), (stage4, 11), (finish, 14))
    for t in range(items + 14):
        for stage, late in stages:
            if 0 <= t - late < items:
                stage(t - late)
        if t == 3:
            weigh(0)
            for n in range(2):
                cbuf[p, n] = jnp.sum(cacc[n].T, axis=0, keepdims=True)
            each(lambda d: cnt_copy(d).start())
        if t == items - 1:
            each(cnt_wait)
            csend[...] = jnp.sum(cbuf[:, 1], axis=0)
            count_back.start()
            number = (lax.broadcasted_iota(jnp.int32, (4, BLOCK), 0) + 1).astype(F32)
            lognorm[...] = log_sums(0, number, lane_of(0))
        if t == items + 4:
            count_back.wait_recv()
            count = jnp.sum(cbuf[:, 0], axis=0) + cret[...]
            ccol[...] = jnp.broadcast_to(count, (BLOCK, width)).T

    old = cent[0, mine_rows, :].astype(F32)
    denom = ccol[mine_rows, 0:1] + 1.0
    updated = (tot[...] + old) / denom
    newc[...] = updated
    move = jnp.sqrt(jnp.sum(jnp.square(updated - old), axis=1, keepdims=True) + 1.0)
    moves = jnp.broadcast_to(move, (own, BLOCK))
    pa[p] = jnp.max(moves, axis=0, keepdims=True)

    def pa_copy(d):
        return rcopy(pa.at[p], pa.at[p], pa_s.at[d], pa_r.at[d], {"dp": dp_at(d)})

    def pa_wait(d):
        src = lax.rem(p + 16 - d, 16)
        rcopy(pa.at[src], pa.at[src], pa_s.at[d], pa_r.at[d], {"dp": src}).wait_recv()

    each(lambda d: pa_copy(d).start())
    tall = jnp.concatenate([moves, jnp.zeros((BLOCK - own, BLOCK), F32)], axis=0)
    shift[...] = tall.T[0:1, :]

    slice_copy.wait_send()
    count_back.wait_send()
    for h in range(2):
        for way in range(2):
            full_copy(way, h).wait_send()
            for j in range(2):
                sel_copy(way, j, h).wait_send()
        for n in range(2):
            for i in range(3):
                part_copy(i, n, h).wait_send()
    for n in range(items):
        for way in range(2):
            for copy in (copy1, copy3, copy4):
                copy(n, way).wait_send()
            for late in (False, True):
                copy2(n, way, late).wait_send()
    for i in range(each_set):
        back_copy(i).wait_send()
    for h in range(2):
        home_copy(h).wait_send()

    def sent(d):
        for copy in (code_copy, spread_copy, cnt_copy):
            copy(d).wait_send()

    each(sent)
    for one in stats(0) + stats(1):
        stat_copy(*one, False).wait_send()

    each(pa_wait)
    peaks[m] = jnp.max(pa[...], axis=0)

    def pb_copy(d):
        return rcopy(peaks.at[m], peaks.at[m], pb_s.at[d], pb_r.at[d], {"mp": mp_at(d)})

    def pb_wait(d):
        src = lax.rem(m + 16 - d, 16)
        rcopy(peaks.at[src], peaks.at[src], pb_s.at[d], pb_r.at[d], {"mp": src}).wait_recv()

    each(lambda d: pb_copy(d).start())
    each(lambda d: pa_copy(d).wait_send())
    each(pb_wait)
    each(lambda d: pb_copy(d).wait_send())


def outputs(made, width, logs, peaks, lower, newc, shift, lognorm, newlow):
    newc[...] = made[...]
    shift[...] = width[:, : shift.shape[1]]
    lognorm[...] = logs[...]
    for s in range(16):
        newlow[s : s + 1, :] = lower[s : s + 1, :] - jnp.concatenate([peaks[s]] * 4, axis=1)


def on_device(data_rows, centroids, block_mask, lower_bound):
    rows, feat = data_rows.shape
    blocks = rows // BLOCK
    width = centroids.shape[0]
    half = feat // 2
    own = width // 16
    items = 2 * (feat // 256)
    dma = pltpu.SemaphoreType.DMA
    vmem = pltpu.VMEM
    made, movement, log_norm, peaks = pl.pallas_call(
        kernel,
        name="kmeans_step",
        out_shape=(
            jax.ShapeDtypeStruct((own, feat), F32),
            jax.ShapeDtypeStruct((1, BLOCK), F32),
            jax.ShapeDtypeStruct((blocks, BLOCK), F32),
            jax.ShapeDtypeStruct((16, 1, BLOCK), F32),
        ),
        in_specs=[pl.BlockSpec(memory_space=pl.ANY)] * 3,
        out_specs=[pl.BlockSpec(memory_space=vmem)] * 4,
        scratch_shapes=[
            vmem((2, rows, half), BF16),
            vmem((2, width, feat), BF16),
            vmem((blocks, 16), jnp.int32),
            vmem((2, 2, rows, half), BF16),
            vmem((2, 2, 8 * BLOCK, half), BF16),
            vmem((3, 2, 2, BLOCK, half), BF16),
            vmem((2, 2, 2, BLOCK, half), BF16),
            vmem((8, 4, 4, own, 256), F32),
            vmem((2, width, 8 * BLOCK), BF16),
            vmem((8, 4, 4, own, 256), F32),
            vmem((items, 2, 2, own, 256), BF16),
            vmem((items, 2, 2, own, 256), BF16),
            vmem((items, 2, 4, own, 256), F32),
            vmem((items, 2, own // 2, 256), F32),
            vmem((items, 2, own, 256), F32),
            vmem((8, own, 256), F32),
            vmem((8, own, 256), F32),
            vmem((2, 4, 4, own, BLOCK), F32),
            vmem((own, feat), F32),
            vmem((4, BLOCK), F32),
            vmem((16, 1, 16), F32),
            vmem((16, 8, 2, BLOCK), F32),
            vmem((16, 8, 2, BLOCK), F32),
            vmem((8, 2, BLOCK), F32),
            vmem((2, 4, 2, BLOCK), F32),
            vmem((2, width, BLOCK), F32),
            vmem((2, width, BLOCK), F32),
            vmem((16, 2, 1, width), F32),
            vmem((1, width), F32),
            vmem((1, width), F32),
            vmem((width, BLOCK), F32),
            vmem((16, 1, BLOCK), F32),
            dma((4,)),
            dma((16,)),
            dma((16,)),
            dma((1,)),
            dma((1,)),
            dma((16,)),
            dma((16,)),
            dma((2, 2)),
            dma((2, 2)),
            dma((3, 2, 2)),
            dma((3, 2, 2)),
            dma((2, 2, 2)),
            dma((2, 2, 2)),
            dma((2, 16)),
            dma((2, 16)),
            dma((16,)),
            dma((16,)),
            *[dma((items, 2)) for _ in range(10)],
            dma((8,)),
            dma((8,)),
            dma((1,)),
            dma((1,)),
            dma((2,)),
            dma((2,)),
            *[dma((16,)) for _ in range(4)],
        ],
        compiler_params=pltpu.CompilerParams(
            collective_id=0, has_side_effects=True, vmem_limit_bytes=66_000_000
        ),
    )(data_rows, centroids, block_mask.T)
    updated, movement, log_norm, new_lower = pl.pallas_call(
        outputs,
        name="outputs",
        out_shape=(
            jax.ShapeDtypeStruct(made.shape, F32),
            jax.ShapeDtypeStruct((1, own), F32),
            jax.ShapeDtypeStruct(log_norm.shape, F32),
            jax.ShapeDtypeStruct(lower_bound.shape, F32),
        ),
        in_specs=[pl.BlockSpec(memory_space=vmem)] * 5,
        out_specs=[pl.BlockSpec(memory_space=vmem)] * 4,
    )(made, movement, log_norm, peaks, lower_bound)
    return updated, movement.reshape(-1), log_norm.reshape(-1), new_lower


def solution(mesh):
    in_specs = (
        P(("dp", "mp"), None),
        P("mp", None),
        P(None, ("dp", "mp")),
        P(None, ("dp", "mp")),
    )
    out_specs = (
        P(("mp", "dp"), None),
        P(("mp", "dp")),
        P(("dp", "mp")),
        P(None, ("dp", "mp")),
    )
    return jax.shard_map(
        on_device, mesh=mesh, in_specs=in_specs, out_specs=out_specs, check_vma=False
    )
```

```python
import functools
import math

import jax
import jax.numpy as jnp
from jax import lax
from jax.experimental import pallas as pl
from jax.experimental.pallas import tpu as pltpu
from jax.sharding import PartitionSpec as P

BLOCK = 128
MESH = pl.DeviceIdType.MESH
NEG = -1e30
F32 = jnp.float32
BF16 = jnp.bfloat16


def rcopy(src, dst, ssem, rsem, dev):
    return pltpu.make_async_remote_copy(
        src_ref=src,
        dst_ref=dst,
        send_sem=ssem,
        recv_sem=rsem,
        device_id=dev,
        device_id_type=MESH,
    )


def kernel(
    data_in,
    cent_in,
    mask_in,
    newc,
    shift,
    lognorm,
    peaks,
    data,
    cent,
    mask,
    full,
    got,
    part,
    selb,
    sc,
    wt,
    sums,
    s1,
    r1,
    r2,
    r3,
    r4,
    te,
    re,
    rz,
    tot,
    cm,
    cv,
    ct,
    st,
    tops,
    nrm,
    cnorm,
    cacc,
    cbuf,
    csend,
    cret,
    ccol,
    pa,
    load_s,
    code_s,
    code_r,
    cs_s,
    cs_r,
    bc_s,
    bc_r,
    full_s,
    full_r,
    part_s,
    part_r,
    sel_s,
    sel_r,
    stat_s,
    stat_r,
    cnt_s,
    cnt_r,
    r1_s,
    r1_r,
    r2_s,
    r2_r,
    r3_s,
    r3_r,
    r4_s,
    r4_r,
    r5_s,
    r5_r,
    ret_s,
    ret_r,
    cret_s,
    cret_r,
    rz_s,
    rz_r,
    pa_s,
    pa_r,
    pb_s,
    pb_r,
):
    half = data.shape[2]
    feat = 2 * half
    width = cent.shape[1]
    own = width // 16
    sharp = 4.0 / math.sqrt(feat)
    p = lax.axis_index("dp")
    m = lax.axis_index("mp")
    z, c = m // 2, lax.rem(m, 2)
    y, x = p // 4, lax.rem(p, 4)
    sign = 1 - 2 * c
    step = (1, -1)
    reach = ((0, 1, -1, 2), (0, 1, -1, -2))
    mine_rows = pl.ds(pl.multiple_of(p * own, own), own)

    def chip(k):
        return lax.rem(z + sign * k + 16, 8)

    def lane(j):
        return c if j == 0 else 1 - c

    def lane_of(j):
        return pl.ds(lane(j), 1)

    def at(k, j):
        return chip(k) * 2 + lane(j)

    def dev(k, j):
        return {"mp": at(k, j)}

    def host(n, k, j):
        if n == 0:
            return at(k, j)
        return at(k + 3, 0) if j == 0 else at(k - 3, 1)

    def slot(n, h, pos, j):
        return got.at[n, h, (pos * 2 + j) * BLOCK : (pos * 2 + j + 1) * BLOCK, :]

    def mp_at(d):
        return lax.rem(m + d, 16)

    def dp_at(d):
        return lax.rem(p + d, 16)

    def each(body):
        lax.fori_loop(1, 16, lambda d, _: (body(d), _)[1], 0)

    barrier = pltpu.get_barrier_semaphore()

    def greet(d):
        pl.semaphore_signal(barrier, inc=1, device_id={"mp": mp_at(d)}, device_id_type=MESH)
        pl.semaphore_signal(barrier, inc=1, device_id={"dp": dp_at(d)}, device_id_type=MESH)

    loads = [pltpu.make_async_copy(mask_in, mask, load_s.at[0])]
    for h in range(2):
        src = data_in.at[:, h * half : (h + 1) * half]
        loads.append(pltpu.make_async_copy(src, data.at[h], load_s.at[1 + h]))
    loads.append(pltpu.make_async_copy(cent_in, cent.at[0], load_s.at[3]))
    for load in loads:
        load.start()
    each(greet)

    loads[0].wait()
    label = (lax.broadcasted_iota(jnp.int32, mask.shape, 0) + 1).astype(F32)
    code = jnp.sum(mask[...].astype(F32) * label, axis=0, keepdims=True)
    cv[m] = code
    shards = lax.broadcasted_iota(jnp.int32, code.shape, 1)
    for n in range(2):
        for j in range(2):
            here = jnp.where(shards == host(n, 0, j), code, 0.0)
            here = jnp.sum(here, axis=1, keepdims=True)
            cm[2 * n + j : 2 * n + j + 1, :] = jnp.broadcast_to(here, (1, BLOCK))
    for load in loads[1:]:
        load.wait()
    pl.semaphore_wait(barrier, 30)

    def code_copy(d):
        return rcopy(cv.at[m], cv.at[m], code_s.at[d], code_r.at[d], {"mp": mp_at(d)})

    def code_wait(d):
        src = lax.rem(m + 16 - d, 16)
        rcopy(cv.at[src], cv.at[src], code_s.at[d], code_r.at[d], {"mp": src}).wait_recv()

    slice_copy = rcopy(cent.at[0, mine_rows], cent.at[1, mine_rows], cs_s.at[0], cs_r.at[0], dev(-3, 0))

    def spread_copy(d):
        ref = cent.at[1, mine_rows]
        return rcopy(ref, ref, bc_s.at[d], bc_r.at[d], {"dp": dp_at(d)})

    def spread_wait(d):
        src = lax.rem(p + 16 - d, 16)
        ref = cent.at[1, pl.ds(pl.multiple_of(src * own, own), own)]
        rcopy(ref, ref, bc_s.at[d], bc_r.at[d], {"dp": src}).wait_recv()

    def full_copy(way, h):
        return rcopy(
            data.at[h], full.at[way, h], full_s.at[way, h], full_r.at[way, h], dev(step[way], 0)
        )

    each(lambda d: code_copy(d).start())
    slice_copy.start()
    for h in range(2):
        for way in range(2):
            full_copy(way, h).start()

    def choose(dst, src, code):
        code = jnp.broadcast_to(code, (BLOCK, BLOCK)).astype(BF16)
        for lanes in range(0, half, BLOCK):
            cols = slice(lanes, lanes + BLOCK)
            out = src[0:BLOCK, cols]
            for b in range(1, src.shape[0] // BLOCK):
                here = code == jnp.asarray(b + 1, BF16)
                out = jnp.where(here, src[b * BLOCK : (b + 1) * BLOCK, cols], out)
            dst[:, cols] = out

    def part_copy(i, n, h):
        return rcopy(
            part.at[i, n, h], slot(n, h, i, 1), part_s.at[i, n, h], part_r.at[i, n, h], dev(0, 1)
        )

    for n in range(2):
        for h in range(2):
            choose(part.at[0, n, h], data.at[h], cm[2 * n + 1 : 2 * n + 2, :])
            choose(slot(n, h, 0, 0), data.at[h], cm[2 * n : 2 * n + 1, :])
    for n in range(2):
        for h in range(2):
            part_copy(0, n, h).start()

    def norms_of(n):
        square = jnp.square(cent[n].astype(F32))
        square = jnp.sum(square, axis=1, keepdims=True)
        cnorm[n] = jnp.broadcast_to(square, cnorm.shape[1:])

    norms_of(0)

    each(code_wait)
    codes = cv[:, 0, :]
    for s in range(16):
        column = jnp.broadcast_to(codes[:, s : s + 1], (16, BLOCK))
        for zg in range(8):
            ct[s, zg] = column[2 * zg : 2 * zg + 2]

    slice_copy.wait_recv()
    each(lambda d: spread_copy(d).start())

    def code_of(k, j, shard):
        return ct[shard, chip(k), lane_of(j), :]

    def row_of(pos, n):
        return (1, 0, 2, 3)[pos] * 2 + n

    def product(n, pos, h):
        return lax.dot_general(
            cent[n, :, h * half : (h + 1) * half],
            got[n, h, pos * 256 : (pos + 1) * 256, :],
            (((1,), (1,)), ((), ())),
            preferred_element_type=F32,
        )

    def weigh_up(n, pos, prod):
        score = sharp * (2.0 * prod - cnorm[n, :, 0:1])
        best = jnp.max(score, axis=0, keepdims=True)
        power = jnp.exp(score - best)
        sc[n * 4 + pos] = power.reshape(sc.shape[1:])
        whole = best + jnp.log(jnp.sum(power, axis=0, keepdims=True))
        row = row_of(pos, n)
        for j in range(2):
            valid = code_of(reach[n][pos], j, host(n, 0, 0)) > 0.0
            lanes = slice(j * BLOCK, (j + 1) * BLOCK)
            tops[row, lane_of(j), :] = best[:, lanes]
            st[m, row, lane_of(j), :] = jnp.where(valid, whole[:, lanes], NEG)

    def scores(n, pos):
        weigh_up(n, pos, product(n, pos, 0) + product(n, pos, 1))

    def keep(way, h):
        k = -step[way]
        for n in range(2):
            choose(part.at[1 + way, n, h], full.at[way, h], code_of(k, 0, host(n, 0, 1)))
            choose(slot(n, h, 2 - way, 0), full.at[way, h], code_of(k, 0, host(n, 0, 0)))

    def sel_copy(way, j, h):
        n = 1 if way == j else 0
        return rcopy(
            selb.at[way, j, h],
            slot(n, h, 3, j),
            sel_s.at[way, j, h],
            sel_r.at[way, j, h],
            dev(step[way], j),
        )

    def select(way, j, h):
        n = 1 if way == j else 0
        code = code_of(-step[way], 0, host(n, step[way], j))
        choose(selb.at[way, j, h], full.at[way, h], code)

    for h in range(2):
        for way in range(2):
            full_copy(way, h).wait_recv()
            for j in range(2):
                select(way, j, h)
            keep(way, h)
            for j in (way, 1 - way)[: 2 - h]:
                sel_copy(way, j, h).start()
            for n in range(2):
                part_copy(1 + way, n, h).start()
        if h == 0:
            for hh in range(2):
                part_copy(0, 0, hh).wait_recv()
            scores(0, 0)
    for pos in (1, 2):
        for h in range(2):
            part_copy(pos, 0, h).wait_recv()
        scores(0, pos)
    each(spread_wait)
    norms_of(1)
    for pos in range(3):
        for h in range(2):
            part_copy(pos, 1, h).wait_recv()
        scores(1, pos)

    early = {0: (0, 6), 1: (0, 6), -1: (0, 6), 2: (0, 4), -2: (2, 6), 3: (0, 2), -3: (4, 6)}
    groups = (early, {k: (7, 8) for k in (-3, -2, -1, 0, 4)}, {k: (6, 7) for k in range(5)})
    peers = [(k, j) for k in range(-3, 5) for j in range(2) if (k, j) != (0, 0)]

    def stat_copy(n, k, j, came):
        rows = groups[n][k]
        src = m if not came else at(-k, 0) if j == 0 else at(k, 1)
        ref, i = st.at[src, rows[0] : rows[1]], (k + 3) * 2 + j
        return rcopy(ref, ref, stat_s.at[n, i], stat_r.at[n, i], {"mp": src} if came else dev(k, j))

    def stats(n):
        return [(n, k, j) for k, j in peers if k in groups[n]]

    for one in stats(0):
        stat_copy(*one, False).start()
    for way in range(2):
        sel_copy(way, 1 - way, 1).start()
    for h in range(2):
        for n in (1, 0):
            for way in range(2):
                sel_copy(way, way if n == 1 else 1 - way, h).wait_recv()
            prod = product(n, 3, h)
            if h == 0:
                sc[n * 4 + 3] = prod.reshape(sc.shape[1:])
            else:
                weigh_up(n, 3, sc[n * 4 + 3].reshape(width, 256) + prod)
                if n == 1:
                    for one in stats(1):
                        stat_copy(*one, False).start()
    for one in stats(2):
        stat_copy(*one, False).start()
    for one in stats(0) + stats(1) + stats(2):
        stat_copy(*one, True).wait_recv()

    def log_sum(pieces):
        top = functools.reduce(jnp.maximum, pieces)
        ceiling = jnp.maximum(top, 0.0)
        total = functools.reduce(jnp.add, [jnp.exp(piece - ceiling) for piece in pieces])
        return ceiling + jnp.log(jnp.exp(-ceiling) + total)

    near = {0: 0, 1: 1, 7: 2, 2: 3}
    afar = {0: 0, 1: 1, 7: 2, 6: 3}

    def log_sums(k, mine, lanes):
        pieces = []
        for q in range(-3, 5):
            for j in range(2):
                turn = 1 - 2 * j
                d = turn * (k - q) % 8
                who, row = at(q, j), 0
                if d in near:
                    row = row_of(near[d], 0)
                else:
                    who, row = at(q - 3 * turn, j), row_of(afar[(d + 3) % 8], 1)
                here = ct[at(q, j), chip(k), lanes, :] == mine
                pieces.append(jnp.where(here, st[who, row, lanes, :], NEG))
        return log_sum(pieces)

    for n in range(2):
        for pos in range(4):
            k = reach[n][pos]
            nrm[n, pos] = log_sums(k, ct[host(n, 0, 0), chip(k)], slice(0, 2))

    def weigh(n):
        for pos in range(4):
            k = reach[n][pos]
            for j in range(2):
                cols = slice(j * BLOCK, (j + 1) * BLOCK)
                gap = tops[row_of(pos, n), lane_of(j), :] - nrm[n, pos, lane_of(j), :]
                scale = jnp.where(code_of(k, j, host(n, 0, 0)) > 0.0, jnp.exp(gap), 0.0)
                power = sc[n * 4 + pos, :, :, :, cols].reshape(width, BLOCK)
                weight = power * scale
                if pos == 0 and j == 0:
                    cacc[n] = weight
                else:
                    cacc[n] += weight
                wt[n, :, pos * 256 + j * BLOCK : pos * 256 + (j + 1) * BLOCK] = weight.astype(BF16)

    weigh(1)

    each_set = 2 * (half // 256)
    items = 2 * each_set
    held = (sc, sums)
    first = (x, y)
    second = (y, x)

    def dp_dev(a, b):
        return {"dp": lax.rem(y + a + 4, 4) * 4 + lax.rem(x + b + 4, 4)}

    def first_dev(h, d):
        return dp_dev(0, d) if h == 0 else dp_dev(d, 0)

    def second_dev(h, d):
        return dp_dev(d, 0) if h == 0 else dp_dev(0, d)

    def plus(v, d):
        return lax.rem(v + d + 4, 4)

    last_q = half // 256 - 1

    def item(n):
        i = n % each_set
        h, q = i % 2, i // 2
        if n < each_set:
            q = (q + last_q) % (last_q + 1)
        return (1 if n < each_set else 0), 2 * q + h, h, q

    def half_rows(way):
        return pl.ds(way * (own // 2), own // 2)

    def wide(n):
        return pl.ds(0, BLOCK if n < 2 else 256)

    def direct(n):
        return n >= items - 2

    def copy1(n, way):
        h, cols = item(n)[2], wide(n)
        src, dst = s1.at[n, way, :, :, cols], r1.at[n, way, :, :, cols]
        return rcopy(src, dst, r1_s.at[n, way], r1_r.at[n, way], first_dev(h, step[way]))

    def copy2(n, way, late):
        (e, i, h, q), cols = item(n), wide(n)
        some = slice(0, 2) if late == (way == 0) else slice(2, 4)
        src = held[e].at[i, plus(first[h], step[way]), some, :, cols]
        dst = r2.at[n, way, some, :, cols]
        sems = (r2_s, r2_r) if late else (r5_s, r5_r)
        return rcopy(src, dst, sems[0].at[n, way], sems[1].at[n, way], first_dev(h, step[way]))

    def copy3(n, way):
        (e, i, h, q), cols = item(n), wide(n)
        src = held[e].at[i, first[h], plus(second[h], 2), half_rows(way), cols]
        dst = r3.at[n, way, :, cols]
        hops = 2 if direct(n) else step[way]
        return rcopy(src, dst, r3_s.at[n, way], r3_r.at[n, way], second_dev(h, hops))

    def copy4(n, way):
        (e, i, h, q), cols = item(n), wide(n)
        src = held[e].at[i, first[h], plus(second[h], step[way]), :, cols]
        dst = r4.at[n, way, :, cols]
        return rcopy(src, dst, r4_s.at[n, way], r4_r.at[n, way], second_dev(h, step[way]))

    def back_copy(i):
        cols = wide(0 if i // 2 == last_q else items)
        src, dst = te.at[i, :, cols], re.at[i, :, cols]
        return rcopy(src, dst, ret_s.at[i], ret_r.at[i], dev(3, 0))

    def home_copy(h):
        src = sums.at[2 * last_q + h, :, :, :, BLOCK:256]
        return rcopy(src, rz.at[h], rz_s.at[h], rz_r.at[h], dev(3, 0))

    def stage1(n):
        e, i, h, q = item(n)
        out = jnp.dot(wt[e], got[e, h, :, q * 256 : (q + 1) * 256], preferred_element_type=F32)
        for owner in range(16):
            yy, xx = owner // 4, owner % 4
            a, b = (xx, yy) if h == 0 else (yy, xx)
            held[e][i, a, b] = out[owner * own : (owner + 1) * own]
        if n >= items - 2:
            home_copy(h).wait_recv()
            held[e][i, :, :, :, BLOCK:256] += rz[h]
        for way in range(2):
            s1[n, way] = held[e][i, plus(first[h], 2), 2 * way : 2 * way + 2].astype(BF16)
        for way in range(2):
            copy1(n, way).start()
        for way in range(2):
            copy2(n, way, False).start()
        if n < 2:
            home_copy(h).start()

    def stage2(n):
        (e, i, h, q), cols = item(n), wide(n)
        for way in range(2):
            copy1(n, way).wait_recv()
            a = plus(first[h], step[way])
            held[e][i, a, 2 * way : 2 * way + 2, :, cols] += r1[n, way, :, :, cols].astype(F32)
            copy2(n, way, True).start()

    def stage3(n):
        (e, i, h, q), cols = item(n), wide(n)
        for way in range(2):
            copy2(n, way, False).wait_recv()
            copy2(n, way, True).wait_recv()
        held[e][i, first[h], :, :, cols] += r2[n, 0, :, :, cols] + r2[n, 1, :, :, cols]
        for way in range(2):
            copy3(n, way).start()
        if direct(n):
            for way in range(2):
                copy4(n, way).start()

    def stage4(n):
        if direct(n):
            return
        (e, i, h, q), cols = item(n), wide(n)
        for way in range(2):
            copy3(n, way).wait_recv()
            b = plus(second[h], step[way])
            held[e][i, first[h], b, half_rows(way), cols] += r3[n, way, :, cols]
            copy4(n, way).start()

    def finish(n):
        (e, i, h, q), cols = item(n), wide(n)
        for way in range(2):
            copy4(n, way).wait_recv()
            if direct(n):
                copy3(n, way).wait_recv()
        value = held[e][i, first[h], second[h], :, cols] + r4[n, 0, :, cols] + r4[n, 1, :, cols]
        if direct(n):
            value = value + jnp.concatenate([r3[n, 0], r3[n, 1]], axis=0)
        if e == 1:
            te[i, :, cols] = value
            back_copy(i).start()
        else:
            back_copy(i).wait_recv()
            start = h * half + q * 256
            tot[:, start : start + 256] = value
            had = BLOCK if q == last_q else 256
            tot[:, start : start + had] += re[i, :, :had]

    def cnt_copy(d):
        return rcopy(cbuf.at[p], cbuf.at[p], cnt_s.at[d], cnt_r.at[d], {"dp": dp_at(d)})

    def cnt_wait(d):
        src = lax.rem(p + 16 - d, 16)
        rcopy(cbuf.at[src], cbuf.at[src], cnt_s.at[d], cnt_r.at[d], {"dp": src}).wait_recv()

    count_back = rcopy(csend, cret, cret_s.at[0], cret_r.at[0], dev(3, 0))

    stages = ((stage1, 0), (stage2, 4), (stage3, 8), (stage4, 11), (finish, 14))
    for t in range(items + 14):
        for stage, late in stages:
            if 0 <= t - late < items:
                stage(t - late)
        if t == 3:
            weigh(0)
            for n in range(2):
                cbuf[p, n] = jnp.sum(cacc[n].T, axis=0, keepdims=True)
            each(lambda d: cnt_copy(d).start())
        if t == items - 1:
            each(cnt_wait)
            csend[...] = jnp.sum(cbuf[:, 1], axis=0)
            count_back.start()
            number = (lax.broadcasted_iota(jnp.int32, (4, BLOCK), 0) + 1).astype(F32)
            lognorm[...] = log_sums(0, number, lane_of(0))
        if t == items + 4:
            count_back.wait_recv()
            count = jnp.sum(cbuf[:, 0], axis=0) + cret[...]
            ccol[...] = jnp.broadcast_to(count, (BLOCK, width)).T

    old = cent[0, mine_rows, :].astype(F32)
    denom = ccol[mine_rows, 0:1] + 1.0
    updated = (tot[...] + old) / denom
    newc[...] = updated
    move = jnp.sqrt(jnp.sum(jnp.square(updated - old), axis=1, keepdims=True) + 1.0)
    moves = jnp.broadcast_to(move, (own, BLOCK))
    pa[p] = jnp.max(moves, axis=0, keepdims=True)

    def pa_copy(d):
        return rcopy(pa.at[p], pa.at[p], pa_s.at[d], pa_r.at[d], {"dp": dp_at(d)})

    def pa_wait(d):
        src = lax.rem(p + 16 - d, 16)
        rcopy(pa.at[src], pa.at[src], pa_s.at[d], pa_r.at[d], {"dp": src}).wait_recv()

    each(lambda d: pa_copy(d).start())
    tall = jnp.concatenate([moves, jnp.zeros((BLOCK - own, BLOCK), F32)], axis=0)
    shift[...] = tall.T[0:1, :]

    slice_copy.wait_send()
    count_back.wait_send()
    for h in range(2):
        for way in range(2):
            full_copy(way, h).wait_send()
            for j in range(2):
                sel_copy(way, j, h).wait_send()
        for n in range(2):
            for i in range(3):
                part_copy(i, n, h).wait_send()
    for n in range(items):
        for way in range(2):
            for copy in (copy1, copy3, copy4):
                copy(n, way).wait_send()
            for late in (False, True):
                copy2(n, way, late).wait_send()
    for i in range(each_set):
        back_copy(i).wait_send()
    for h in range(2):
        home_copy(h).wait_send()

    def sent(d):
        for copy in (code_copy, spread_copy, cnt_copy):
            copy(d).wait_send()

    each(sent)
    for one in stats(0) + stats(1) + stats(2):
        stat_copy(*one, False).wait_send()

    each(pa_wait)
    peaks[m] = jnp.max(pa[...], axis=0)

    def pb_copy(d):
        return rcopy(peaks.at[m], peaks.at[m], pb_s.at[d], pb_r.at[d], {"mp": mp_at(d)})

    def pb_wait(d):
        src = lax.rem(m + 16 - d, 16)
        rcopy(peaks.at[src], peaks.at[src], pb_s.at[d], pb_r.at[d], {"mp": src}).wait_recv()

    each(lambda d: pb_copy(d).start())
    each(lambda d: pa_copy(d).wait_send())
    each(pb_wait)
    each(lambda d: pb_copy(d).wait_send())


def outputs(made, width, logs, peaks, lower, newc, shift, lognorm, newlow):
    newc[...] = made[...]
    shift[...] = width[:, : shift.shape[1]]
    lognorm[...] = logs[...]
    for s in range(16):
        newlow[s : s + 1, :] = lower[s : s + 1, :] - jnp.concatenate([peaks[s]] * 4, axis=1)


def on_device(data_rows, centroids, block_mask, lower_bound):
    rows, feat = data_rows.shape
    blocks = rows // BLOCK
    width = centroids.shape[0]
    half = feat // 2
    own = width // 16
    items = 2 * (feat // 256)
    dma = pltpu.SemaphoreType.DMA
    vmem = pltpu.VMEM
    made, movement, log_norm, peaks = pl.pallas_call(
        kernel,
        name="kmeans_step",
        out_shape=(
            jax.ShapeDtypeStruct((own, feat), F32),
            jax.ShapeDtypeStruct((1, BLOCK), F32),
            jax.ShapeDtypeStruct((blocks, BLOCK), F32),
            jax.ShapeDtypeStruct((16, 1, BLOCK), F32),
        ),
        in_specs=[pl.BlockSpec(memory_space=pl.ANY)] * 3,
        out_specs=[pl.BlockSpec(memory_space=vmem)] * 4,
        scratch_shapes=[
            vmem((2, rows, half), BF16),
            vmem((2, width, feat), BF16),
            vmem((blocks, 16), jnp.int32),
            vmem((2, 2, rows, half), BF16),
            vmem((2, 2, 8 * BLOCK, half), BF16),
            vmem((3, 2, 2, BLOCK, half), BF16),
            vmem((2, 2, 2, BLOCK, half), BF16),
            vmem((8, 4, 4, own, 256), F32),
            vmem((2, width, 8 * BLOCK), BF16),
            vmem((8, 4, 4, own, 256), F32),
            vmem((items, 2, 2, own, 256), BF16),
            vmem((items, 2, 2, own, 256), BF16),
            vmem((items, 2, 4, own, 256), F32),
            vmem((items, 2, own // 2, 256), F32),
            vmem((items, 2, own, 256), F32),
            vmem((8, own, 256), F32),
            vmem((8, own, 256), F32),
            vmem((2, 4, 4, own, BLOCK), F32),
            vmem((own, feat), F32),
            vmem((4, BLOCK), F32),
            vmem((16, 1, 16), F32),
            vmem((16, 8, 2, BLOCK), F32),
            vmem((16, 8, 2, BLOCK), F32),
            vmem((8, 2, BLOCK), F32),
            vmem((2, 4, 2, BLOCK), F32),
            vmem((2, width, BLOCK), F32),
            vmem((2, width, BLOCK), F32),
            vmem((16, 2, 1, width), F32),
            vmem((1, width), F32),
            vmem((1, width), F32),
            vmem((width, BLOCK), F32),
            vmem((16, 1, BLOCK), F32),
            dma((4,)),
            dma((16,)),
            dma((16,)),
            dma((1,)),
            dma((1,)),
            dma((16,)),
            dma((16,)),
            dma((2, 2)),
            dma((2, 2)),
            dma((3, 2, 2)),
            dma((3, 2, 2)),
            dma((2, 2, 2)),
            dma((2, 2, 2)),
            dma((3, 16)),
            dma((3, 16)),
            dma((16,)),
            dma((16,)),
            *[dma((items, 2)) for _ in range(10)],
            dma((8,)),
            dma((8,)),
            dma((1,)),
            dma((1,)),
            dma((2,)),
            dma((2,)),
            *[dma((16,)) for _ in range(4)],
        ],
        compiler_params=pltpu.CompilerParams(
            collective_id=0, has_side_effects=True, vmem_limit_bytes=66_000_000
        ),
    )(data_rows, centroids, block_mask.T)
    updated, movement, log_norm, new_lower = pl.pallas_call(
        outputs,
        name="outputs",
        out_shape=(
            jax.ShapeDtypeStruct(made.shape, F32),
            jax.ShapeDtypeStruct((1, own), F32),
            jax.ShapeDtypeStruct(log_norm.shape, F32),
            jax.ShapeDtypeStruct(lower_bound.shape, F32),
        ),
        in_specs=[pl.BlockSpec(memory_space=vmem)] * 5,
        out_specs=[pl.BlockSpec(memory_space=vmem)] * 4,
    )(made, movement, log_norm, peaks, lower_bound)
    return updated, movement.reshape(-1), log_norm.reshape(-1), new_lower


def solution(mesh):
    in_specs = (
        P(("dp", "mp"), None),
        P("mp", None),
        P(None, ("dp", "mp")),
        P(None, ("dp", "mp")),
    )
    out_specs = (
        P(("mp", "dp"), None),
        P(("mp", "dp")),
        P(("dp", "mp")),
        P(None, ("dp", "mp")),
    )
    return jax.shard_map(
        on_device, mesh=mesh, in_specs=in_specs, out_specs=out_specs, check_vma=False
    )
```
